16 devices in a mesh: col: 4 (over z, y), row: 4 (over x, core).
Axes of the slice: x: 2, y: 2, z: 2, core: 2. Of those that a mesh axis runs over, the one named last changes fastest.
Arguments:
- forcing: float32 [2, 192, 192, 256], P(None, 'row', 'col')
- init_guess: float32 [2, 192, 192, 256], P(None, 'row', 'col')
- cell_coef: float32 [2, 192, 192], P(None, 'row', 'col')
- solve_rows: bfloat16 [2, 4, 4, 2304, 3136], P(None, 'row', 'col')
- relax_factor: float32 [2], replicated
Outputs:
- output: float32 [2, 192, 192, 256], P(None, 'row', 'col')
All inputs are finite; a program needn't handle non-finite values.
Results may differ from the reference program's by a relative error of at most 0.00114.
Values are sent between devices in bfloat16 or wider.
A program may use at most 1 GiB of HBM per device.

```python
import jax
import jax.numpy as jnp
from jax import lax

SUBDOMAIN = 48
MARGIN = 4
RHS_PER_SYS = 256
SWEEPS = 4
BLOCK_ROWS = 4
BLOCK_COLS = 4
SYSTEMS = 2

EXT_SIZE = SUBDOMAIN + 2 * MARGIN
GRID_ROWS = BLOCK_ROWS * SUBDOMAIN
GRID_COLS = BLOCK_COLS * SUBDOMAIN


def face_coefs(coef_grid):
    face_x = jnp.concatenate([coef_grid[:1], 0.5 * (coef_grid[:-1] + coef_grid[1:]), coef_grid[-1:]], axis=0)
    face_y = jnp.concatenate([coef_grid[:, :1], 0.5 * (coef_grid[:, :-1] + coef_grid[:, 1:]), coef_grid[:, -1:]], axis=1)
    return face_x, face_y


def apply_op(face_x, face_y, values):
    wide_x = jnp.pad(values, ((1, 1), (0, 0), (0, 0)))
    wide_y = jnp.pad(values, ((0, 0), (1, 1), (0, 0)))
    flux_x = face_x[:, :, None] * (wide_x[1:] - wide_x[:-1])
    flux_y = face_y[:, :, None] * (wide_y[:, 1:] - wide_y[:, :-1])
    return flux_x[:-1] - flux_x[1:] + flux_y[:, :-1] - flux_y[:, 1:]


def subdomain_inverses(coef_grid):
    face_x, face_y = face_coefs(coef_grid)
    diagonal = face_x[:-1] + face_x[1:] + face_y[:, :-1] + face_y[:, 1:]
    diag_pad = jnp.pad(diagonal, MARGIN, constant_values=1.0)
    couple_x = jnp.pad(face_x[1:-1], MARGIN)
    couple_y = jnp.pad(face_y[:, 1:-1], MARGIN)

    def one_block(block_id):
        row_start = (block_id // BLOCK_COLS) * SUBDOMAIN
        col_start = (block_id % BLOCK_COLS) * SUBDOMAIN
        diag_blk = lax.dynamic_slice(diag_pad, (row_start, col_start), (EXT_SIZE, EXT_SIZE)).reshape(-1)
        link_x = lax.dynamic_slice(couple_x, (row_start, col_start), (EXT_SIZE - 1, EXT_SIZE)).reshape(-1)
        link_y = lax.dynamic_slice(couple_y, (row_start, col_start), (EXT_SIZE, EXT_SIZE - 1))
        link_y = jnp.pad(link_y, ((0, 0), (0, 1))).reshape(-1)[:-1]
        local_op = jnp.diag(diag_blk) - jnp.diag(link_x, EXT_SIZE) - jnp.diag(link_x, -EXT_SIZE) - jnp.diag(link_y, 1) - jnp.diag(link_y, -1)
        full_inv = jnp.linalg.inv(local_op)
        own_rows = full_inv.reshape(EXT_SIZE, EXT_SIZE, EXT_SIZE * EXT_SIZE)[MARGIN:MARGIN + SUBDOMAIN, MARGIN:MARGIN + SUBDOMAIN]
        return own_rows.reshape(SUBDOMAIN * SUBDOMAIN, EXT_SIZE * EXT_SIZE)

    blocks = lax.map(one_block, jnp.arange(BLOCK_ROWS * BLOCK_COLS))
    return blocks.reshape(BLOCK_ROWS, BLOCK_COLS, SUBDOMAIN * SUBDOMAIN, EXT_SIZE * EXT_SIZE)


def setup_inputs(seed: int = 0) -> dict:
    base_key = jax.random.key(seed)
    key_f, key_u, key_c, key_w = jax.random.split(base_key, 4)
    grid_shape = (SYSTEMS, GRID_ROWS, GRID_COLS, RHS_PER_SYS)
    forcing = jax.random.normal(key_f, grid_shape, jnp.float32)
    init_guess = 0.5 * jax.random.normal(key_u, grid_shape, jnp.float32)
    cell_coef = jnp.exp(1.2 * jax.random.uniform(key_c, (SYSTEMS, GRID_ROWS, GRID_COLS), jnp.float32, -1.0, 1.0))
    relax_factor = jax.random.uniform(key_w, (SYSTEMS,), jnp.float32, 0.35, 0.6)
    solve_rows = jnp.stack([subdomain_inverses(cell_coef[system]) for system in range(SYSTEMS)]).astype(jnp.bfloat16)
    return {"forcing": forcing, "init_guess": init_guess, "cell_coef": cell_coef, "solve_rows": solve_rows, "relax_factor": relax_factor}


def solve_system(rhs_grid, start_guess, coef_grid, inv_rows, step_size):
    face_x, face_y = face_coefs(coef_grid)
    flat_rows = inv_rows.reshape(BLOCK_ROWS * BLOCK_COLS, SUBDOMAIN * SUBDOMAIN, EXT_SIZE * EXT_SIZE)
    block_ids = jnp.arange(BLOCK_ROWS * BLOCK_COLS)

    def one_sweep(sweep_state, unused):
        approx, residual = sweep_state
        padded = jnp.pad(residual.astype(jnp.bfloat16), ((MARGIN, MARGIN), (MARGIN, MARGIN), (0, 0)))

        def block_solve(operands):
            block_id, block_mat = operands
            row_start = (block_id // BLOCK_COLS) * SUBDOMAIN
            col_start = (block_id % BLOCK_COLS) * SUBDOMAIN
            window = lax.dynamic_slice(padded, (row_start, col_start, 0), (EXT_SIZE, EXT_SIZE, RHS_PER_SYS))
            return jnp.dot(block_mat, window.reshape(EXT_SIZE * EXT_SIZE, RHS_PER_SYS), preferred_element_type=jnp.float32)

        correction = lax.map(block_solve, (block_ids, flat_rows))
        correction = correction.reshape(BLOCK_ROWS, BLOCK_COLS, SUBDOMAIN, SUBDOMAIN, RHS_PER_SYS).transpose(0, 2, 1, 3, 4).reshape(GRID_ROWS, GRID_COLS, RHS_PER_SYS)
        approx = approx + step_size * correction
        residual = residual - step_size * apply_op(face_x, face_y, correction)
        return (approx, residual), None

    residual = rhs_grid - apply_op(face_x, face_y, start_guess)
    (approx, _), _ = lax.scan(one_sweep, (start_guess, residual), None, length=SWEEPS)
    return approx


def reference(forcing, init_guess, cell_coef, solve_rows, relax_factor):
    results = [solve_system(forcing[system], init_guess[system], cell_coef[system], solve_rows[system], relax_factor[system]) for system in range(SYSTEMS)]
    return jnp.stack(results)
```

```python
import jax
import jax.numpy as jnp
from jax import lax
from jax.experimental import pallas as pl
from jax.experimental.pallas import tpu as pltpu
from jax.sharding import PartitionSpec as P

SWEEPS = 4
MESH_ID = pl.DeviceIdType.MESH
NB = 48
MG = 4
EX = NB + 2 * MG
LANES = 128
CHUNKS = 3
S_COPIES = 4
SIDES = ((-1, 0), (1, 0), (0, -1), (0, 1))
OPP_SIDE = (1, 0, 3, 2)
CORNERS = ((-1, -1), (-1, 1), (1, -1), (1, 1))
F32 = jnp.float32
BF16 = jnp.bfloat16


def kernel(f_hbm, u_hbm, c_ref, s_hbm, om_ref, out_hbm,
           S, Z, R, W, U, C, FX, FY, FE, ces, cer, zes, zer, frs, frr, crs, crr,
           sem_f, sem_u, sem_s, sem_o, sem_cs, sem_cr, sem_zs, sem_zr,
           sem_fs, sem_fr, sem_ks, sem_kr):
    row = lax.axis_index("row")
    col = lax.axis_index("col")
    has_side = (row > 0, row < 3, col > 0, col < 3)
    has_corner = tuple(
        jnp.logical_and(has_side[0] if dr < 0 else has_side[1], has_side[2] if dc < 0 else has_side[3])
        for dr, dc in CORNERS)

    def dev(delta):
        return {"row": row + delta[0], "col": col + delta[1]}

    def ext_col(j):
        return pl.ds(EX * MG + j, NB, stride=EX)

    def own_row(i):
        return pl.ds(EX * (MG + i) + MG, NB)

    def u_copy(s, h):
        return pltpu.make_async_copy(u_hbm.at[s, :, :, pl.ds(h * LANES, LANES)], Z.at[s, h, pl.ds(1, NB), pl.ds(8, NB), :], sem_u.at[s, h])

    def f_copy(s, h):
        return pltpu.make_async_copy(f_hbm.at[s, :, :, pl.ds(h * LANES, LANES)], U.at[s, h], sem_f.at[s, h])

    rows_per = NB * NB // CHUNKS
    k_per = EX * EX // S_COPIES

    def s_copy(s, m):
        return pltpu.make_async_copy(s_hbm.at[s, pl.ds(m * k_per, k_per), :], S.at[s, pl.ds(m * k_per, k_per), :], sem_s.at[s, m])

    def o_copy(s, h, m):
        g = NB // CHUNKS
        return pltpu.make_async_copy(U.at[s, h, pl.ds(m * g, g)], out_hbm.at[s, pl.ds(m * g, g), :, pl.ds(h * LANES, LANES)], sem_o.at[s, h, m])

    for s in range(2):
        for h in range(2):
            u_copy(s, h).start()
    for s in range(2):
        for h in range(2):
            f_copy(s, h).start()
    for s in range(2):
        for m in range(S_COPIES):
            s_copy(s, m).start()

    barrier = pltpu.get_barrier_semaphore()
    n_side = sum(h.astype(jnp.int32) for h in has_side) + sum(h.astype(jnp.int32) for h in has_corner)
    for cond, delta in zip(has_side + has_corner, SIDES + CORNERS):
        @pl.when(cond)
        def _(delta=delta):
            pl.semaphore_signal(barrier, inc=1, device_id=dev(delta), device_id_type=MESH_ID)

    for s in range(2):
        c_t = c_ref[s].T
        for i in range(NB):
            C[s, i, 8:EX, :] = jnp.broadcast_to(c_t[:, i:i + 1], (NB, LANES))

    zero_row = jnp.zeros((64, LANES), F32)

    def zero_z(s, h):
        Z[s, h, 0, :, :] = zero_row
        Z[s, h, 49, :, :] = zero_row

        @pl.loop(1, 49)
        def _(i):
            Z[s, h, i, 0:8, :] = jnp.zeros((8, LANES), F32)
            Z[s, h, i, EX:64, :] = jnp.zeros((8, LANES), F32)

    for s in range(2):
        for h in range(2):
            zero_z(s, h)

    @pl.loop(0, 57)
    def _(i):
        for s in range(2):
            for h in range(2):
                R[s, h, pl.ds(pl.multiple_of(EX * i, 8), EX), :] = jnp.zeros((EX, LANES), F32)

    for s in range(2):
        ces[0, s] = C[s, 0, 8:EX, :]
        ces[1, s] = C[s, NB - 1, 8:EX, :]
        ces[2, s] = C[s, :, 8, :]
        ces[3, s] = C[s, :, EX - 1, :]

    pl.semaphore_wait(barrier, n_side)

    def c_send(d):
        return pltpu.make_async_remote_copy(ces.at[d], cer.at[OPP_SIDE[d]], sem_cs.at[d], sem_cr.at[OPP_SIDE[d]], device_id=dev(SIDES[d]), device_id_type=MESH_ID)

    def c_recv(d):
        return pltpu.make_async_remote_copy(ces.at[OPP_SIDE[d]], cer.at[d], sem_cs.at[OPP_SIDE[d]], sem_cr.at[d], device_id=dev(SIDES[d]), device_id_type=MESH_ID)

    for d in range(4):
        @pl.when(has_side[d])
        def _(d=d):
            c_send(d).start()

    def z_send(s, d):
        return pltpu.make_async_remote_copy(zes.at[s, d], zer.at[s, OPP_SIDE[d]], sem_zs.at[s, d], sem_zr.at[s, OPP_SIDE[d]], device_id=dev(SIDES[d]), device_id_type=MESH_ID)

    def z_recv(s, d):
        return pltpu.make_async_remote_copy(zes.at[s, OPP_SIDE[d]], zer.at[s, d], sem_zs.at[s, OPP_SIDE[d]], sem_zr.at[s, d], device_id=dev(SIDES[d]), device_id_type=MESH_ID)

    def f_send(s, d):
        return pltpu.make_async_remote_copy(frs.at[s, d], frr.at[s, OPP_SIDE[d]], sem_fs.at[s, d], sem_fr.at[s, OPP_SIDE[d]], device_id=dev(SIDES[d]), device_id_type=MESH_ID)

    def f_recv(s, d):
        return pltpu.make_async_remote_copy(frs.at[s, OPP_SIDE[d]], frr.at[s, d], sem_fs.at[s, OPP_SIDE[d]], sem_fr.at[s, d], device_id=dev(SIDES[d]), device_id_type=MESH_ID)

    def k_send(s, q, p):
        return pltpu.make_async_remote_copy(crs.at[s, q], crr.at[p, s, 3 - q], sem_ks.at[s, q], sem_kr.at[p, s, 3 - q], device_id=dev(CORNERS[q]), device_id_type=MESH_ID)

    def k_recv(s, q, p):
        return pltpu.make_async_remote_copy(crs.at[s, 3 - q], crr.at[p, s, q], sem_ks.at[s, 3 - q], sem_kr.at[p, s, q], device_id=dev(CORNERS[q]), device_id_type=MESH_ID)

    def when_all(conds, body):
        for i, c in enumerate(conds):
            @pl.when(c)
            def _(i=i):
                body(i)

    def send_z_edges(s):
        for h in range(2):
            zes[s, 2, h] = Z[s, h, 1:NB + 1, 8, :]
            zes[s, 3, h] = Z[s, h, 1:NB + 1, EX - 1, :]
        for h in range(2):
            zes[s, 0, h] = Z[s, h, 1, 8:EX, :]
            zes[s, 1, h] = Z[s, h, NB, 8:EX, :]
        for d in (2, 3, 0, 1):
            @pl.when(has_side[d])
            def _(d=d):
                z_send(s, d).start()

    def stencil(s, om, first):
        @pl.loop(0, NB)
        def _(i):
            ax0 = FX[s, i, :, :]
            ax1 = FX[s, i + 1, :, :]
            ay0 = FY[s, i, 0:NB, :]
            ay1 = FY[s, i, 1:NB + 1, :]
            for h in range(2):
                zc = Z[s, h, i + 1, 8:EX, :]
                zl = Z[s, h, i + 1, 7:EX - 1, :]
                zr = Z[s, h, i + 1, 9:EX + 1, :]
                zu = Z[s, h, i, 8:EX, :]
                zd = Z[s, h, i + 2, 8:EX, :]
                av = ax0 * (zc - zu) - ax1 * (zd - zc) + ay0 * (zc - zl) - ay1 * (zr - zc)
                if first:
                    R[s, h, own_row(i), :] = U[s, h, i] - av
                    U[s, h, i] = zc
                else:
                    R[s, h, own_row(i), :] = R[s, h, own_row(i), :] - om * av
                    U[s, h, i] = U[s, h, i] + om * zc

    def edge_fix(s, om):
        def fix(d):
            z_recv(s, d).wait_recv()
            for h in range(2):
                cells = (own_row(0), own_row(NB - 1), ext_col(MG), ext_col(MG + NB - 1))[d]
                R[s, h, cells, :] = R[s, h, cells, :] + om * (FE[s, d] * zer[s, d, h])
        for d in (0, 1, 2, 3):
            @pl.when(has_side[d])
            def _(d=d):
                fix(d)

    def send_frames(s, p):
        for h in range(2):
            lanes = pl.ds(h * LANES, LANES)
            for a in range(MG):
                frs[s, 2, a, :, lanes] = R[s, h, ext_col(MG + a), :].astype(BF16)
                frs[s, 3, a, :, lanes] = R[s, h, ext_col(NB + a), :].astype(BF16)
                frs[s, 0, a, :, lanes] = R[s, h, own_row(a), :].astype(BF16)
                frs[s, 1, a, :, lanes] = R[s, h, own_row(NB - MG + a), :].astype(BF16)
            for q, (dr, dc) in enumerate(CORNERS):
                r0 = MG if dr < 0 else NB
                c0 = 0 if dc < 0 else NB
                tile = [R[s, h, pl.ds(EX * (r0 + a) + c0, 8), :] for a in range(MG)]
                crs[s, q, :, lanes] = jnp.concatenate(tile, axis=0).astype(BF16)
        for d in (2, 3, 0, 1):
            @pl.when(has_side[d])
            def _(d=d):
                f_send(s, d).start()
        when_all(has_corner, lambda q: k_send(s, q, p).start())

    def recv_frames(s, p):
        def side(d):
            f_recv(s, d).wait_recv()
            for h in range(2):
                lanes = pl.ds(h * LANES, LANES)
                for a in range(MG):
                    v = frr[s, d, a, :, lanes].astype(F32)
                    cells = (own_row(a - MG), own_row(NB + a), ext_col(a), ext_col(MG + NB + a))[d]
                    R[s, h, cells, :] = v

        def corner(q):
            k_recv(s, q, p).wait_recv()
            dr, dc = CORNERS[q]
            r0 = 0 if dr < 0 else MG + NB
            for h in range(2):
                v = crr[p, s, q, :, pl.ds(h * LANES, LANES)].astype(F32)
                for a in range(MG):
                    if dc < 0:
                        R[s, h, pl.ds(EX * (r0 + a), 4), :] = v[8 * a:8 * a + 4]
                    else:
                        R[s, h, pl.ds(EX * (r0 + a) + MG + NB, 4), :] = v[8 * a + 4:8 * a + 8]
        when_all(has_side, side)
        when_all(has_corner, corner)

    def wait_frame_sends(s, p):
        when_all(has_side, lambda d: z_send(s, d).wait_send())
        when_all(has_side, lambda d: f_send(s, d).wait_send())
        when_all(has_corner, lambda q: k_send(s, q, p).wait_send())

    def fill_window(s):
        @pl.loop(0, EX // 2)
        def _(t):
            for h in range(2):
                v = R[s, h, pl.ds(pl.multiple_of(2 * EX * t, 16), 2 * EX), :]
                W[s, pl.ds(pl.multiple_of(2 * EX * t, 16), 2 * EX), pl.ds(h * LANES, LANES)] = v.astype(BF16)

    g = NB // CHUNKS

    def matmul(s, m):
        z = lax.dot_general(S[s, :, pl.ds(m * rows_per, rows_per)], W[s], (((0,), (0,)), ((), ())), preferred_element_type=F32)
        return z.reshape(g, NB, 2 * LANES)

    def matmul_to_z(s):
        for m in range(CHUNKS):
            z = matmul(s, m)
            for h in range(2):
                Z[s, h, pl.ds(1 + m * g, g), 8:EX, :] = z[:, :, h * LANES:(h + 1) * LANES]

    for s in range(2):
        for h in range(2):
            u_copy(s, h).wait()
        send_z_edges(s)
    for s in range(2):
        @pl.loop(1, NB)
        def _(i):
            FX[s, i, :, :] = 0.5 * (C[s, i - 1, 8:EX, :] + C[s, i, 8:EX, :])
        C[s, :, 0:8, :] = jnp.zeros((NB, 8, LANES), F32)

        @pl.loop(0, NB)
        def _(i):
            FY[s, i, 0:NB, :] = 0.5 * (C[s, i, 7:EX - 1, :] + C[s, i, 8:EX, :])
    when_all(has_side, lambda d: c_recv(d).wait_recv())
    for s in range(2):
        for d in range(4):
            own = ces[d, s]
            face = jnp.where(has_side[d], 0.5 * (own + cer[d, s]), own)
            if d == 0:
                FX[s, 0, :, :] = face
            elif d == 1:
                FX[s, NB, :, :] = face
            elif d == 2:
                FY[s, :, 0, :] = face
            else:
                FY[s, :, NB, :] = face
            FE[s, d] = face
    for s in range(2):
        for h in range(2):
            f_copy(s, h).wait()
        stencil(s, None, True)
        edge_fix(s, 1.0)
        send_frames(s, 0)

    for s in range(2):
        for m in range(S_COPIES):
            s_copy(s, m).wait()

    @pl.loop(0, SWEEPS - 1)
    def _(k):
        p = lax.rem(k, 2)
        for s in range(2):
            recv_frames(s, p)
            wait_frame_sends(s, p)
            fill_window(s)
            matmul_to_z(s)
            send_z_edges(s)
        for s in range(2):
            om = om_ref[s]
            stencil(s, om, False)
            edge_fix(s, om)
            send_frames(s, 1 - p)

    last = (SWEEPS - 1) % 2
    for s in range(2):
        recv_frames(s, last)
        wait_frame_sends(s, last)
        fill_window(s)
        for m in range(CHUNKS):
            z = matmul(s, m)
            for h in range(2):
                U[s, h, pl.ds(m * g, g)] = U[s, h, pl.ds(m * g, g)] + om_ref[s] * z[:, :, h * LANES:(h + 1) * LANES]
                o_copy(s, h, m).start()
    when_all(has_side, lambda d: c_send(d).wait_send())
    for s in range(2):
        for h in range(2):
            for m in range(CHUNKS):
                o_copy(s, h, m).wait()


def solution(mesh):
    grid_spec = P(None, "row", "col", None)

    def local(forcing, init_guess, cell_coef, solve_rows, relax_factor):
        num_sys, nb, _, rhs = forcing.shape
        s_mat = jnp.swapaxes(solve_rows, 3, 4).reshape(num_sys, solve_rows.shape[-1], nb * nb)
        any_spec = pl.BlockSpec(memory_space=pl.ANY)
        dma = pltpu.SemaphoreType.DMA
        return pl.pallas_call(
            kernel,
            name="schwarz",
            out_shape=jax.ShapeDtypeStruct(forcing.shape, F32),
            in_specs=[any_spec, any_spec, pl.BlockSpec(memory_space=pltpu.VMEM), any_spec, pl.BlockSpec(memory_space=pltpu.SMEM)],
            out_specs=any_spec,
            scratch_shapes=[
                pltpu.VMEM((2, EX * EX, NB * NB), BF16),
                pltpu.VMEM((2, 2, 50, 64, LANES), F32),
                pltpu.VMEM((2, 2, 57 * EX, LANES), F32),
                pltpu.VMEM((2, EX * EX, 2 * LANES), BF16),
                pltpu.VMEM((2, 2, NB, NB, LANES), F32),
                pltpu.VMEM((2, NB, EX, LANES), F32),
                pltpu.VMEM((2, NB + 1, NB, LANES), F32),
                pltpu.VMEM((2, NB, EX, LANES), F32),
                pltpu.VMEM((2, 4, NB, LANES), F32),
                pltpu.VMEM((4, 2, NB, LANES), F32),
                pltpu.VMEM((4, 2, NB, LANES), F32),
                pltpu.VMEM((2, 4, 2, NB, LANES), F32),
                pltpu.VMEM((2, 4, 2, NB, LANES), F32),
                pltpu.VMEM((2, 4, MG, NB, 2 * LANES), BF16),
                pltpu.VMEM((2, 4, MG, NB, 2 * LANES), BF16),
                pltpu.VMEM((2, 4, 32, 2 * LANES), BF16),
                pltpu.VMEM((2, 2, 4, 32, 2 * LANES), BF16),
                dma((2, 2)), dma((2, 2)), dma((2, S_COPIES)), dma((2, 2, CHUNKS)),
                dma((4,)), dma((4,)), dma((2, 4)), dma((2, 4)),
                dma((2, 4)), dma((2, 4)), dma((2, 4)), dma((2, 2, 4)),
            ],
            compiler_params=pltpu.CompilerParams(collective_id=0, has_side_effects=True, vmem_limit_bytes=66_000_000),
            cost_estimate=pl.CostEstimate(flops=30_000_000_000, bytes_accessed=43_000_000, transcendentals=0),
        )(forcing, init_guess, cell_coef, s_mat, relax_factor)

    return jax.shard_map(local, mesh=mesh, in_specs=(grid_spec, grid_spec, P(None, "row", "col"), P(None, "row", "col", None, None), P(None)), out_specs=grid_spec, check_vma=False)
```

```python
import jax
import jax.numpy as jnp
from jax import lax
from jax.experimental import pallas as pl
from jax.experimental.pallas import tpu as pltpu
from jax.sharding import PartitionSpec as P

SWEEPS = 4
MESH_ID = pl.DeviceIdType.MESH
NB = 48
MG = 4
EX = NB + 2 * MG
LANES = 128
CHUNKS = 3
OFF = 4
KI = 24 * 64
KF = EX * EX - KI
SIDES = ((-1, 0), (1, 0), (0, -1), (0, 1))
OPP_SIDE = (1, 0, 3, 2)
CORNERS = ((-1, -1), (-1, 1), (1, -1), (1, 1))
F32 = jnp.float32
BF16 = jnp.bfloat16


def kernel(f_hbm, u_hbm, c_ref, s_hbm, om_ref, out_hbm,
           SI, SA, SF, Z, R, W, U, C, FX, FY, FE, ces, cer, zes, zer, frs, frr, crs, crr,
           sem_f, sem_u, sem_s, sem_o, sem_cs, sem_cr, sem_zs, sem_zr,
           sem_fs, sem_fr, sem_ks, sem_kr, sem_es, sem_er):
    row = lax.axis_index("row")
    col = lax.axis_index("col")
    has_side = (row > 0, row < 3, col > 0, col < 3)
    has_corner = tuple(
        jnp.logical_and(has_side[0] if dr < 0 else has_side[1], has_side[2] if dc < 0 else has_side[3])
        for dr, dc in CORNERS)

    def dev(delta):
        return {"row": row + delta[0], "col": col + delta[1]}

    def ext_col(j):
        return pl.ds(OFF + EX * MG + j, NB, stride=EX)

    def own_row(i):
        return pl.ds(pl.multiple_of(OFF + EX * (MG + i) + MG, 8), NB)

    def u_copy(s, h):
        return pltpu.make_async_copy(u_hbm.at[s, :, :, pl.ds(h * LANES, LANES)], Z.at[s, h, pl.ds(1, NB), pl.ds(8, NB), :], sem_u.at[s, h])

    def f_copy(s, h):
        return pltpu.make_async_copy(f_hbm.at[s, :, :, pl.ds(h * LANES, LANES)], U.at[s, h], sem_f.at[s, h])

    rows_per = NB * NB // CHUNKS

    mid = pl.ds(2, 24)

    def s_copies(s):
        parts = (
            (s_hbm.at[s, mid, pl.ds(1, 2)], SI.at[s, :, pl.ds(0, 2)]),
            (s_hbm.at[s, mid, pl.ds(4, 2)], SI.at[s, :, pl.ds(2, 2)]),
            (s_hbm.at[s, pl.ds(0, 2)], SA.at[s, pl.ds(0, 2)]),
            (s_hbm.at[s, pl.ds(26, 2)], SA.at[s, pl.ds(2, 2)]),
            (s_hbm.at[s, mid, pl.ds(0, 1)], SF.at[s, :, pl.ds(0, 1)]),
            (s_hbm.at[s, mid, pl.ds(3, 1)], SF.at[s, :, pl.ds(1, 1)]),
            (s_hbm.at[s, mid, pl.ds(6, 1)], SF.at[s, :, pl.ds(2, 1)]))
        return [pltpu.make_async_copy(src, dst, sem_s.at[s, m]) for m, (src, dst) in enumerate(parts)]

    def o_copy(s, h, m):
        g = NB // CHUNKS
        return pltpu.make_async_copy(U.at[s, h, pl.ds(m * g, g)], out_hbm.at[s, pl.ds(m * g, g), :, pl.ds(h * LANES, LANES)], sem_o.at[s, h, m])

    for s in range(2):
        for h in range(2):
            u_copy(s, h).start()
    for s in range(2):
        for h in range(2):
            f_copy(s, h).start()
    for s in range(2):
        for cp in s_copies(s):
            cp.start()

    barrier = pltpu.get_barrier_semaphore()
    n_side = sum(h.astype(jnp.int32) for h in has_side) + sum(h.astype(jnp.int32) for h in has_corner)
    for cond, delta in zip(has_side + has_corner, SIDES + CORNERS):
        @pl.when(cond)
        def _(delta=delta):
            pl.semaphore_signal(barrier, inc=1, device_id=dev(delta), device_id_type=MESH_ID)

    for s in range(2):
        c_t = c_ref[s].T
        for i in range(NB):
            C[s, i, 8:EX, :] = jnp.broadcast_to(c_t[:, i:i + 1], (NB, LANES))

    zero_row = jnp.zeros((64, LANES), F32)

    def zero_z(s, h):
        Z[s, h, 0, :, :] = zero_row
        Z[s, h, 49, :, :] = zero_row

        @pl.loop(1, 49)
        def _(i):
            Z[s, h, i, 0:8, :] = jnp.zeros((8, LANES), F32)
            Z[s, h, i, EX:64, :] = jnp.zeros((8, LANES), F32)

    for s in range(2):
        for h in range(2):
            zero_z(s, h)

    @pl.loop(0, 57)
    def _(i):
        for s in range(2):
            for h in range(2):
                R[s, h, pl.ds(pl.multiple_of(EX * i, 8), EX), :] = jnp.zeros((EX, LANES), F32)

    for s in range(2):
        ces[0, s] = C[s, 0, 8:EX, :]
        ces[1, s] = C[s, NB - 1, 8:EX, :]
        ces[2, s] = C[s, :, 8, :]
        ces[3, s] = C[s, :, EX - 1, :]

    pl.semaphore_wait(barrier, n_side)

    def c_send(d):
        return pltpu.make_async_remote_copy(ces.at[d], cer.at[OPP_SIDE[d]], sem_cs.at[d], sem_cr.at[OPP_SIDE[d]], device_id=dev(SIDES[d]), device_id_type=MESH_ID)

    def c_recv(d):
        return pltpu.make_async_remote_copy(ces.at[OPP_SIDE[d]], cer.at[d], sem_cs.at[OPP_SIDE[d]], sem_cr.at[d], device_id=dev(SIDES[d]), device_id_type=MESH_ID)

    for d in range(4):
        @pl.when(has_side[d])
        def _(d=d):
            c_send(d).start()

    def remote(src, dst, ssem, rsem, delta):
        return pltpu.make_async_remote_copy(src, dst, ssem, rsem, device_id=dev(delta), device_id_type=MESH_ID)

    def z_copy(s, d, slot):
        return remote(zes.at[s, d], zer.at[s, slot], sem_zs.at[s, d], sem_zr.at[s, slot], SIDES[d])

    def z_send(s, d):
        return z_copy(s, d, OPP_SIDE[d])

    def z_recv(s, d):
        return z_copy(s, OPP_SIDE[d], d)

    def early_layers(d):
        return pl.ds(1, 3) if d == 2 else pl.ds(0, 3)

    def late_layers(d):
        return (pl.ds(0, 4), pl.ds(0, 4), pl.ds(0, 1), pl.ds(3, 1))[d]

    def e_copy(s, d, slot, p):
        lay = early_layers(d)
        return remote(frs.at[s, d, lay], frr.at[p, s, slot, lay], sem_es.at[s, d], sem_er.at[p, s, slot], SIDES[d])

    def f_copy_remote(s, d, slot, p):
        lay = late_layers(d)
        return remote(frs.at[s, d, lay], frr.at[p, s, slot, lay], sem_fs.at[s, d], sem_fr.at[p, s, slot], SIDES[d])

    def k_copy(s, q, slot, p):
        return remote(crs.at[s, q], crr.at[p, s, slot], sem_ks.at[s, q], sem_kr.at[p, s, slot], CORNERS[q])

    def when_all(conds, body, order=None):
        for i in (order or range(len(conds))):
            @pl.when(conds[i])
            def _(i=i):
                body(i)

    COLS = (2, 3)
    ROWS = (0, 1)

    def send_z_edges(s, again):
        if again:
            when_all(has_side, lambda d: z_send(s, d).wait_send())
        for h in range(2):
            zes[s, 2, h] = Z[s, h, 1:NB + 1, 8, :]
            zes[s, 3, h] = Z[s, h, 1:NB + 1, EX - 1, :]
        for h in range(2):
            zes[s, 0, h] = Z[s, h, 1, 8:EX, :]
            zes[s, 1, h] = Z[s, h, NB, 8:EX, :]
        when_all(has_side, lambda d: z_send(s, d).start(), COLS + ROWS)

    def stencil(s, om, first):
        @pl.loop(0, NB)
        def _(i):
            ax0 = FX[s, i, :, :]
            ax1 = FX[s, i + 1, :, :]
            ay0 = FY[s, i, 0:NB, :]
            ay1 = FY[s, i, 1:NB + 1, :]
            for h in range(2):
                zc = Z[s, h, i + 1, 8:EX, :]
                zl = Z[s, h, i + 1, 7:EX - 1, :]
                zr = Z[s, h, i + 1, 9:EX + 1, :]
                zu = Z[s, h, i, 8:EX, :]
                zd = Z[s, h, i + 2, 8:EX, :]
                av = ax0 * (zc - zu) - ax1 * (zd - zc) + ay0 * (zc - zl) - ay1 * (zr - zc)
                if first:
                    R[s, h, own_row(i), :] = U[s, h, i] - av
                    U[s, h, i] = zc
                else:
                    R[s, h, own_row(i), :] = R[s, h, own_row(i), :] - om * av
                    U[s, h, i] = U[s, h, i] + om * zc

    def edge_fix(s, om, sides):
        def fix(d):
            z_recv(s, d).wait_recv()
            for h in range(2):
                cells = (own_row(0), own_row(NB - 1), ext_col(MG), ext_col(MG + NB - 1))[d]
                R[s, h, cells, :] = R[s, h, cells, :] + om * (FE[s, d] * zer[s, d, h])
        when_all(has_side, fix, sides)

    def pack_col(s, h, d, a):
        first = MG if d == 2 else NB
        frs[s, d, a, :, pl.ds(h * LANES, LANES)] = R[s, h, ext_col(first + a), :].astype(BF16)

    def send_early(s, p, again):
        if again:
            when_all(has_side, lambda d: e_copy(s, d, OPP_SIDE[d], p).wait_send(), COLS)
        for d in COLS:
            for h in range(2):
                for a in ((1, 2, 3) if d == 2 else (0, 1, 2)):
                    pack_col(s, h, d, a)
        when_all(has_side, lambda d: e_copy(s, d, OPP_SIDE[d], p).start(), COLS)

    def send_late(s, p, again):
        if again:
            when_all(has_side, lambda d: f_copy_remote(s, d, OPP_SIDE[d], p).wait_send())
            when_all(has_corner, lambda q: k_copy(s, q, 3 - q, p).wait_send())
        for h in range(2):
            lanes = pl.ds(h * LANES, LANES)
            pack_col(s, h, 2, 0)
            pack_col(s, h, 3, 3)
            for a in range(MG):
                frs[s, 0, a, :, lanes] = R[s, h, own_row(a), :].astype(BF16)
                frs[s, 1, a, :, lanes] = R[s, h, own_row(NB - MG + a), :].astype(BF16)
            for q, (dr, dc) in enumerate(CORNERS):
                r0 = MG if dr < 0 else NB
                c0 = 0 if dc < 0 else NB
                tile = [R[s, h, pl.ds(OFF + EX * (r0 + a) + c0, 8), :] for a in range(MG)]
                crs[s, q, :, lanes] = jnp.concatenate(tile, axis=0).astype(BF16)
        when_all(has_side, lambda d: f_copy_remote(s, d, OPP_SIDE[d], p).start(), COLS + ROWS)
        when_all(has_corner, lambda q: k_copy(s, q, 3 - q, p).start())

    def recv_frames(s, p):
        def side(d):
            if d in COLS:
                e_copy(s, OPP_SIDE[d], d, p).wait_recv()
            f_copy_remote(s, OPP_SIDE[d], d, p).wait_recv()
            for h in range(2):
                lanes = pl.ds(h * LANES, LANES)
                for a in range(MG):
                    v = frr[p, s, d, a, :, lanes].astype(F32)
                    cells = (own_row(a - MG), own_row(NB + a), ext_col(a), ext_col(MG + NB + a))[d]
                    R[s, h, cells, :] = v

        def corner(q):
            k_copy(s, 3 - q, q, p).wait_recv()
            dr, dc = CORNERS[q]
            r0 = 0 if dr < 0 else MG + NB
            for h in range(2):
                v = crr[p, s, q, :, pl.ds(h * LANES, LANES)].astype(F32)
                for a in range(MG):
                    if dc < 0:
                        R[s, h, pl.ds(OFF + EX * (r0 + a), 4), :] = v[8 * a:8 * a + 4]
                    else:
                        R[s, h, pl.ds(OFF + EX * (r0 + a) + MG + NB, 4), :] = v[8 * a + 4:8 * a + 8]
        when_all(has_side, side)
        when_all(has_corner, corner)

    def pair_rows(s, h, t):
        return R[s, h, pl.ds(2 * EX * t + OFF, 2 * EX), :].astype(BF16)

    def fill_inner(s):
        @pl.loop(2, 26)
        def _(t):
            for h in range(2):
                v = pair_rows(s, h, t)
                for n, u in enumerate((1, 2, 4, 5)):
                    W[s, pl.ds(pl.multiple_of(64 * (t - 2) + 16 * n, 16), 16), pl.ds(h * LANES, LANES)] = v[16 * u:16 * u + 16]

    def fill_frame(s):
        @pl.loop(2, 26)
        def _(t):
            for h in range(2):
                v = pair_rows(s, h, t)
                for n, u in enumerate((0, 3, 6)):
                    W[s, pl.ds(pl.multiple_of(KI + 448 + 48 * (t - 2) + 16 * n, 16), 16), pl.ds(h * LANES, LANES)] = v[16 * u:16 * u + 16]
        for h in range(2):
            for n, t in enumerate((0, 1, 26, 27)):
                W[s, pl.ds(KI + 112 * n, 112), pl.ds(h * LANES, LANES)] = pair_rows(s, h, t)

    g = NB // CHUNKS

    def matmul(s, m, parts, k0):
        cells = pl.ds(m * rows_per, rows_per)
        lhs = [p[s, :, :, :, cells].reshape(-1, rows_per) for p in parts]
        lhs = jnp.concatenate(lhs, axis=0) if len(lhs) > 1 else lhs[0]
        z = lax.dot_general(lhs, W[s, pl.ds(k0, lhs.shape[0]), :], (((0,), (0,)), ((), ())), preferred_element_type=F32)
        return z.reshape(g, NB, 2 * LANES)

    def inner_product(s):
        fill_inner(s)
        for m in range(CHUNKS):
            z = matmul(s, m, (SI,), 0)
            for h in range(2):
                Z[s, h, pl.ds(1 + m * g, g), 8:EX, :] = z[:, :, h * LANES:(h + 1) * LANES]

    def frame_product(s, m):
        z = matmul(s, m, (SA, SF), KI)
        return [Z[s, h, pl.ds(1 + m * g, g), 8:EX, :] + z[:, :, h * LANES:(h + 1) * LANES] for h in range(2)]

    for s in range(2):
        for h in range(2):
            u_copy(s, h).wait()
        send_z_edges(s, False)
    for s in range(2):
        @pl.loop(1, NB)
        def _(i):
            FX[s, i, :, :] = 0.5 * (C[s, i - 1, 8:EX, :] + C[s, i, 8:EX, :])
        C[s, :, 0:8, :] = jnp.zeros((NB, 8, LANES), F32)

        @pl.loop(0, NB)
        def _(i):
            FY[s, i, 0:NB, :] = 0.5 * (C[s, i, 7:EX - 1, :] + C[s, i, 8:EX, :])
    when_all(has_side, lambda d: c_recv(d).wait_recv())
    for s in range(2):
        for d in range(4):
            own = ces[d, s]
            face = jnp.where(has_side[d], 0.5 * (own + cer[d, s]), own)
            if d == 0:
                FX[s, 0, :, :] = face
            elif d == 1:
                FX[s, NB, :, :] = face
            elif d == 2:
                FY[s, :, 0, :] = face
            else:
                FY[s, :, NB, :] = face
            FE[s, d] = face
    for s in range(2):
        for h in range(2):
            f_copy(s, h).wait()
        stencil(s, None, True)
    for s in range(2):
        edge_fix(s, 1.0, ROWS)
        send_early(s, 0, False)
    for s in range(2):
        edge_fix(s, 1.0, COLS)
        send_late(s, 0, False)

    for s in range(2):
        for cp in s_copies(s):
            cp.wait()
        inner_product(s)

    def half_sweep(s, k, p_in, other, p_other, fix_other):
        recv_frames(s, p_in)
        fill_frame(s)
        for m in range(CHUNKS):
            z = frame_product(s, m)
            for h in range(2):
                Z[s, h, pl.ds(1 + m * g, g), 8:EX, :] = z[h]
            if m == 1:
                late(other, p_other, fix_other)
        send_z_edges(s, True)
        stencil(s, om_ref[s], False)

    def late(s, p, wanted):
        @pl.when(wanted)
        def _():
            edge_fix(s, om_ref[s], COLS)
            send_late(s, p, True)

    @pl.loop(0, SWEEPS - 1)
    def _(k):
        p = lax.rem(k, 2)
        half_sweep(0, k, p, 1, p, k > 0)

        @pl.when(k > 0)
        def _():
            inner_product(1)
        edge_fix(0, om_ref[0], ROWS)
        send_early(0, 1 - p, True)
        half_sweep(1, k, p, 0, 1 - p, k >= 0)
        inner_product(0)
        edge_fix(1, om_ref[1], ROWS)
        send_early(1, 1 - p, True)

    last = (SWEEPS - 1) % 2

    def finish(s, m):
        z = frame_product(s, m)
        for h in range(2):
            U[s, h, pl.ds(m * g, g)] = U[s, h, pl.ds(m * g, g)] + om_ref[s] * z[h]
            o_copy(s, h, m).start()

    recv_frames(0, last)
    fill_frame(0)
    for m in range(CHUNKS):
        finish(0, m)
        if m == 1:
            late(1, last, row >= 0)
    inner_product(1)
    recv_frames(1, last)
    fill_frame(1)
    for m in range(CHUNKS):
        finish(1, m)
    when_all(has_side, lambda d: c_send(d).wait_send())
    for s in range(2):
        when_all(has_side, lambda d: z_send(s, d).wait_send())
        when_all(has_side, lambda d: e_copy(s, d, OPP_SIDE[d], last).wait_send(), COLS)
        when_all(has_side, lambda d: f_copy_remote(s, d, OPP_SIDE[d], last).wait_send())
        when_all(has_corner, lambda q: k_copy(s, q, 3 - q, last).wait_send())
        for h in range(2):
            for m in range(CHUNKS):
                o_copy(s, h, m).wait()


def solution(mesh):
    grid_spec = P(None, "row", "col", None)

    def local(forcing, init_guess, cell_coef, solve_rows, relax_factor):
        num_sys, nb, _, rhs = forcing.shape
        s_mat = jnp.swapaxes(solve_rows, 3, 4).reshape(num_sys, EX // 2, 7, 16, nb * nb)
        any_spec = pl.BlockSpec(memory_space=pl.ANY)
        dma = pltpu.SemaphoreType.DMA
        return pl.pallas_call(
            kernel,
            name="schwarz",
            out_shape=jax.ShapeDtypeStruct(forcing.shape, F32),
            in_specs=[any_spec, any_spec, pl.BlockSpec(memory_space=pltpu.VMEM), any_spec, pl.BlockSpec(memory_space=pltpu.SMEM)],
            out_specs=any_spec,
            scratch_shapes=[
                pltpu.VMEM((2, 24, 4, 16, NB * NB), BF16),
                pltpu.VMEM((2, 4, 7, 16, NB * NB), BF16),
                pltpu.VMEM((2, 24, 3, 16, NB * NB), BF16),
                pltpu.VMEM((2, 2, 50, 64, LANES), F32),
                pltpu.VMEM((2, 2, 57 * EX, LANES), F32),
                pltpu.VMEM((2, EX * EX, 2 * LANES), BF16),
                pltpu.VMEM((2, 2, NB, NB, LANES), F32),
                pltpu.VMEM((2, NB, EX, LANES), F32),
                pltpu.VMEM((2, NB + 1, NB, LANES), F32),
                pltpu.VMEM((2, NB, EX, LANES), F32),
                pltpu.VMEM((2, 4, NB, LANES), F32),
                pltpu.VMEM((4, 2, NB, LANES), F32),
                pltpu.VMEM((4, 2, NB, LANES), F32),
                pltpu.VMEM((2, 4, 2, NB, LANES), F32),
                pltpu.VMEM((2, 4, 2, NB, LANES), F32),
                pltpu.VMEM((2, 4, MG, NB, 2 * LANES), BF16),
                pltpu.VMEM((2, 2, 4, MG, NB, 2 * LANES), BF16),
                pltpu.VMEM((2, 4, 32, 2 * LANES), BF16),
                pltpu.VMEM((2, 2, 4, 32, 2 * LANES), BF16),
                dma((2, 2)), dma((2, 2)), dma((2, 7)), dma((2, 2, CHUNKS)),
                dma((4,)), dma((4,)), dma((2, 4)), dma((2, 4)),
                dma((2, 4)), dma((2, 2, 4)), dma((2, 4)), dma((2, 2, 4)), dma((2, 4)), dma((2, 2, 4)),
            ],
            compiler_params=pltpu.CompilerParams(collective_id=0, has_side_effects=True, vmem_limit_bytes=66_000_000),
            cost_estimate=pl.CostEstimate(flops=30_000_000_000, bytes_accessed=43_000_000, transcendentals=0),
        )(forcing, init_guess, cell_coef, s_mat, relax_factor)

    return jax.shard_map(local, mesh=mesh, in_specs=(grid_spec, grid_spec, P(None, "row", "col"), P(None, "row", "col", None, None), P(None)), out_specs=grid_spec, check_vma=False)
```

```python
import jax
import jax.numpy as jnp
from jax import lax
from jax.experimental import pallas as pl
from jax.experimental.pallas import tpu as pltpu
from jax.sharding import PartitionSpec as P

SWEEPS = 4
MESH_ID = pl.DeviceIdType.MESH
NB = 48
MG = 4
EX = NB + 2 * MG
LANES = 128
CHUNKS = 3
LATE_AT = 1
OFF = 4
KI = 24 * 64
KF = EX * EX - KI
SIDES = ((-1, 0), (1, 0), (0, -1), (0, 1))
OPP_SIDE = (1, 0, 3, 2)
CORNERS = ((-1, -1), (-1, 1), (1, -1), (1, 1))
F32 = jnp.float32
BF16 = jnp.bfloat16


def kernel(f_hbm, u_hbm, c_ref, s_hbm, om_ref, out_hbm,
           SI, SA, SF, Z, R, W, U, FX, FY, FE, ces, cer, zes, zer, frs, frr, crs, crr,
           sem_f, sem_u, sem_s, sem_o, sem_cs, sem_cr, sem_zs, sem_zr,
           sem_fs, sem_fr, sem_ks, sem_kr, sem_es, sem_er):
    row = lax.axis_index("row")
    col = lax.axis_index("col")
    has_side = (row > 0, row < 3, col > 0, col < 3)
    has_corner = tuple(
        jnp.logical_and(has_side[0] if dr < 0 else has_side[1], has_side[2] if dc < 0 else has_side[3])
        for dr, dc in CORNERS)

    def dev(delta):
        return {"row": row + delta[0], "col": col + delta[1]}

    def ext_col(j):
        return pl.ds(OFF + EX * MG + j, NB, stride=EX)

    def own_row(i):
        start = OFF + EX * (MG + i) + MG
        return pl.ds(start if isinstance(i, int) else pl.multiple_of(start, 8), NB)

    def u_copy(s, h):
        return pltpu.make_async_copy(u_hbm.at[s, :, :, pl.ds(h * LANES, LANES)], Z.at[s, h, pl.ds(1, NB), pl.ds(8, NB), :], sem_u.at[s, h])

    def f_copy(s, h):
        return pltpu.make_async_copy(f_hbm.at[s, :, :, pl.ds(h * LANES, LANES)], U.at[s, h], sem_f.at[s, h])

    rows_per = NB * NB // CHUNKS

    mid = pl.ds(2, 24)

    def s_copies(s, inner):
        parts = (
            (s_hbm.at[s, mid, pl.ds(1, 2)], SI.at[s, :, pl.ds(0, 2)]),
            (s_hbm.at[s, mid, pl.ds(4, 2)], SI.at[s, :, pl.ds(2, 2)]),
            (s_hbm.at[s, pl.ds(0, 2)], SA.at[s, pl.ds(0, 2)]),
            (s_hbm.at[s, pl.ds(26, 2)], SA.at[s, pl.ds(2, 2)]),
            (s_hbm.at[s, mid, pl.ds(0, 1)], SF.at[s, :, pl.ds(0, 1)]),
            (s_hbm.at[s, mid, pl.ds(3, 1)], SF.at[s, :, pl.ds(1, 1)]),
            (s_hbm.at[s, mid, pl.ds(6, 1)], SF.at[s, :, pl.ds(2, 1)]))
        return [pltpu.make_async_copy(src, dst, sem_s.at[s, m]) for m, (src, dst) in enumerate(parts) if (m < 2) == inner]

    def o_copy(s, h, m):
        g = NB // CHUNKS
        return pltpu.make_async_copy(U.at[s, h, pl.ds(m * g, g)], out_hbm.at[s, pl.ds(m * g, g), :, pl.ds(h * LANES, LANES)], sem_o.at[s, h, m])

    for s in range(2):
        for h in range(2):
            u_copy(s, h).start()
    for s in range(2):
        for h in range(2):
            f_copy(s, h).start()
    for first in (True, False):
        for s in range(2):
            for cp in s_copies(s, first):
                cp.start()

    barrier = pltpu.get_barrier_semaphore()
    n_side = sum(h.astype(jnp.int32) for h in has_side) + sum(h.astype(jnp.int32) for h in has_corner)
    for cond, delta in zip(has_side + has_corner, SIDES + CORNERS):
        @pl.when(cond)
        def _(delta=delta):
            pl.semaphore_signal(barrier, inc=1, device_id=dev(delta), device_id_type=MESH_ID)

    for s in range(2):
        c_t = c_ref[s].T
        for i in range(NB):
            R[s, 0, pl.ds(EX * i + 8, NB), :] = jnp.broadcast_to(c_t[:, i:i + 1], (NB, LANES))

    zero_row = jnp.zeros((64, LANES), F32)

    def zero_z(s, h):
        Z[s, h, 0, :, :] = zero_row
        Z[s, h, 49, :, :] = zero_row

        @pl.loop(1, 49)
        def _(i):
            Z[s, h, i, 0:8, :] = jnp.zeros((8, LANES), F32)
            Z[s, h, i, EX:64, :] = jnp.zeros((8, LANES), F32)

    for s in range(2):
        for h in range(2):
            zero_z(s, h)

    for d in range(4):
        @pl.when(jnp.logical_not(has_side[d]))
        def _(d=d):
            for s in range(2):
                zer[s, d] = jnp.zeros((2, NB, LANES), F32)
                for p in range(2):
                    frr[p, s, d] = jnp.zeros((MG, NB, 2 * LANES), BF16)
    for q in range(4):
        @pl.when(jnp.logical_not(has_corner[q]))
        def _(q=q):
            for s in range(2):
                for p in range(2):
                    crr[p, s, q] = jnp.zeros((32, 2 * LANES), BF16)

    for s in range(2):
        ces[0, s] = R[s, 0, pl.ds(8, NB), :]
        ces[1, s] = R[s, 0, pl.ds(EX * (NB - 1) + 8, NB), :]
        ces[2, s] = R[s, 0, pl.ds(8, NB, stride=EX), :]
        ces[3, s] = R[s, 0, pl.ds(EX - 1, NB, stride=EX), :]

    pl.semaphore_wait(barrier, n_side)

    def c_send(d):
        return pltpu.make_async_remote_copy(ces.at[d], cer.at[OPP_SIDE[d]], sem_cs.at[d], sem_cr.at[OPP_SIDE[d]], device_id=dev(SIDES[d]), device_id_type=MESH_ID)

    def c_recv(d):
        return pltpu.make_async_remote_copy(ces.at[OPP_SIDE[d]], cer.at[d], sem_cs.at[OPP_SIDE[d]], sem_cr.at[d], device_id=dev(SIDES[d]), device_id_type=MESH_ID)

    for d in range(4):
        @pl.when(has_side[d])
        def _(d=d):
            c_send(d).start()

    def remote(src, dst, ssem, rsem, delta):
        return pltpu.make_async_remote_copy(src, dst, ssem, rsem, device_id=dev(delta), device_id_type=MESH_ID)

    def z_copy(s, d, slot):
        return remote(zes.at[s, d], zer.at[s, slot], sem_zs.at[s, d], sem_zr.at[s, slot], SIDES[d])

    def z_send(s, d):
        return z_copy(s, d, OPP_SIDE[d])

    def z_recv(s, d):
        return z_copy(s, OPP_SIDE[d], d)

    def early_layers(d):
        return pl.ds(1, 3) if d == 2 else pl.ds(0, 3)

    def late_layers(d):
        return (pl.ds(0, 4), pl.ds(0, 4), pl.ds(0, 1), pl.ds(3, 1))[d]

    def e_copy(s, d, slot, p):
        lay = early_layers(d)
        return remote(frs.at[s, d, lay], frr.at[p, s, slot, lay], sem_es.at[s, d], sem_er.at[p, s, slot], SIDES[d])

    def f_copy_remote(s, d, slot, p):
        lay = late_layers(d)
        return remote(frs.at[s, d, lay], frr.at[p, s, slot, lay], sem_fs.at[s, d], sem_fr.at[p, s, slot], SIDES[d])

    def k_copy(s, q, slot, p):
        return remote(crs.at[s, q], crr.at[p, s, slot], sem_ks.at[s, q], sem_kr.at[p, s, slot], CORNERS[q])

    def when_all(conds, body, order=None):
        for i in (order or range(len(conds))):
            @pl.when(conds[i])
            def _(i=i):
                body(i)

    COLS = (2, 3)
    ROWS = (0, 1)

    def send_z_edges(s, again):
        if again:
            when_all(has_side, lambda d: z_send(s, d).wait_send())
        for h in range(2):
            zes[s, 2, h] = Z[s, h, 1:NB + 1, 8, :]
            zes[s, 3, h] = Z[s, h, 1:NB + 1, EX - 1, :]
        for h in range(2):
            zes[s, 0, h] = Z[s, h, 1, 8:EX, :]
            zes[s, 1, h] = Z[s, h, NB, 8:EX, :]
        when_all(has_side, lambda d: z_send(s, d).start(), COLS + ROWS)

    def stencil(s, om, first):
        @pl.loop(0, NB)
        def _(i):
            ax0 = FX[s, i, :, :]
            ax1 = FX[s, i + 1, :, :]
            ay0 = FY[s, i, 0:NB, :]
            ay1 = FY[s, i, 1:NB + 1, :]
            for h in range(2):
                zc = Z[s, h, i + 1, 8:EX, :]
                zl = Z[s, h, i + 1, 7:EX - 1, :]
                zr = Z[s, h, i + 1, 9:EX + 1, :]
                zu = Z[s, h, i, 8:EX, :]
                zd = Z[s, h, i + 2, 8:EX, :]
                av = ax0 * (zc - zu) - ax1 * (zd - zc) + ay0 * (zc - zl) - ay1 * (zr - zc)
                if first:
                    R[s, h, own_row(i), :] = U[s, h, i] - av
                    U[s, h, i] = zc
                else:
                    R[s, h, own_row(i), :] = R[s, h, own_row(i), :] - om * av
                    U[s, h, i] = U[s, h, i] + om * zc

    def stencil_rows(s, om, rows):
        for h in range(2):
            zc = Z[s, h, rows[0] + 1, 8:EX, :]
            flux = FX[s, rows[0], :, :] * (zc - Z[s, h, rows[0], 8:EX, :])
            for i in rows:
                zd = Z[s, h, i + 2, 8:EX, :]
                down = FX[s, i + 1, :, :] * (zd - zc)
                side = FY[s, i, 0:NB, :] * (zc - Z[s, h, i + 1, 7:EX - 1, :]) - FY[s, i, 1:NB + 1, :] * (Z[s, h, i + 1, 9:EX + 1, :] - zc)
                R[s, h, own_row(i), :] = R[s, h, own_row(i), :] - om * ((flux - down) + side)
                U[s, h, i] = U[s, h, i] + om * zc
                flux, zc = down, zd

    def wait_z(s, sides):
        when_all(has_side, lambda d: z_recv(s, d).wait_recv(), sides)

    def edge_fix(s, om, sides):
        for d in sides:
            for h in range(2):
                cells = (own_row(0), own_row(NB - 1), ext_col(MG), ext_col(MG + NB - 1))[d]
                R[s, h, cells, :] = R[s, h, cells, :] + om * (FE[s, d] * zer[s, d, h])

    def pack_col(s, h, d, a):
        first = MG if d == 2 else NB
        frs[s, d, a, :, pl.ds(h * LANES, LANES)] = R[s, h, ext_col(first + a), :].astype(BF16)

    def send_early(s, p, again):
        if again:
            when_all(has_side, lambda d: e_copy(s, d, OPP_SIDE[d], p).wait_send(), COLS)
        for d in COLS:
            for h in range(2):
                for a in ((1, 2, 3) if d == 2 else (0, 1, 2)):
                    pack_col(s, h, d, a)
        when_all(has_side, lambda d: e_copy(s, d, OPP_SIDE[d], p).start(), COLS)

    def send_late(s, p, again):
        if again:
            when_all(has_side, lambda d: f_copy_remote(s, d, OPP_SIDE[d], p).wait_send())
            when_all(has_corner, lambda q: k_copy(s, q, 3 - q, p).wait_send())
        for h in range(2):
            lanes = pl.ds(h * LANES, LANES)
            pack_col(s, h, 2, 0)
            pack_col(s, h, 3, 3)
            for a in range(MG):
                frs[s, 0, a, :, lanes] = R[s, h, own_row(a), :].astype(BF16)
                frs[s, 1, a, :, lanes] = R[s, h, own_row(NB - MG + a), :].astype(BF16)
            for q, (dr, dc) in enumerate(CORNERS):
                r0 = MG if dr < 0 else NB
                c0 = 0 if dc < 0 else NB
                tile = [R[s, h, pl.ds(OFF + EX * (r0 + a) + c0, 8), :] for a in range(MG)]
                crs[s, q, :, lanes] = jnp.concatenate(tile, axis=0).astype(BF16)
        when_all(has_side, lambda d: f_copy_remote(s, d, OPP_SIDE[d], p).start(), COLS + ROWS)
        when_all(has_corner, lambda q: k_copy(s, q, 3 - q, p).start())

    def wait_frames(s, p):
        when_all(has_side, lambda d: e_copy(s, OPP_SIDE[d], d, p).wait_recv(), COLS)
        when_all(has_side, lambda d: f_copy_remote(s, OPP_SIDE[d], d, p).wait_recv())
        when_all(has_corner, lambda q: k_copy(s, 3 - q, q, p).wait_recv())

    def scatter_frames(s, p):
        for d in range(4):
            for h in range(2):
                for a in range(MG):
                    cells = (own_row(a - MG), own_row(NB + a), ext_col(a), ext_col(MG + NB + a))[d]
                    R[s, h, cells, :] = frr[p, s, d, a, :, pl.ds(h * LANES, LANES)].astype(F32)
        for q, (dr, dc) in enumerate(CORNERS):
            r0 = 0 if dr < 0 else MG + NB
            for h in range(2):
                v = crr[p, s, q, :, pl.ds(h * LANES, LANES)].astype(F32)
                for a in range(MG):
                    if dc < 0:
                        R[s, h, pl.ds(OFF + EX * (r0 + a), 4), :] = v[8 * a:8 * a + 4]
                    else:
                        R[s, h, pl.ds(OFF + EX * (r0 + a) + MG + NB, 4), :] = v[8 * a + 4:8 * a + 8]

    def pair_rows(s, h, t):
        return R[s, h, pl.ds(2 * EX * t + OFF, 2 * EX), :].astype(BF16)

    def fill(s, t, tile, n, base):
        for h in range(2):
            v = R[s, h, pl.ds(2 * EX * t + 16 * tile + OFF, 16 * n), :].astype(BF16)
            W[s, pl.ds(base, 16 * n), pl.ds(h * LANES, LANES)] = v

    def fill_inner(s):
        for t in range(2, 26):
            fill(s, t, 1, 2, 64 * (t - 2))
            fill(s, t, 4, 2, 64 * (t - 2) + 32)

    def fill_frame(s):
        fill(s, 0, 0, 14, KI)
        fill(s, 26, 0, 14, KI + 224)
        for t in range(2, 26):
            for n, u in enumerate((0, 3, 6)):
                fill(s, t, u, 1, KI + 448 + 48 * (t - 2) + 16 * n)

    g = NB // CHUNKS

    def matmul(s, m, parts, k0):
        cells = pl.ds(m * rows_per, rows_per)
        lhs = [p[s, :, :, :, cells].reshape(-1, rows_per) for p in parts]
        lhs = jnp.concatenate(lhs, axis=0) if len(lhs) > 1 else lhs[0]
        z = lax.dot_general(lhs, W[s, pl.ds(k0, lhs.shape[0]), :], (((0,), (0,)), ((), ())), preferred_element_type=F32)
        return z.reshape(g, NB, 2 * LANES)

    def inner_product(s, other=None):
        fill_inner(s)
        for m in range(CHUNKS):
            if other is not None:
                stencil_rows(other, om_ref[other], range(m * g, (m + 1) * g))
            z = matmul(s, m, (SI,), 0)
            for h in range(2):
                Z[s, h, pl.ds(1 + m * g, g), 8:EX, :] = z[:, :, h * LANES:(h + 1) * LANES]

    def frame_product(s, m):
        z = matmul(s, m, (SA, SF), KI)
        return [Z[s, h, pl.ds(1 + m * g, g), 8:EX, :] + z[:, :, h * LANES:(h + 1) * LANES] for h in range(2)]

    for s in range(2):
        for h in range(2):
            u_copy(s, h).wait()
        send_z_edges(s, False)
    for s in range(2):
        for i in range(NB):
            R[s, 0, pl.ds(EX * i, 8), :] = jnp.zeros((8, LANES), F32)

        @pl.loop(0, NB)
        def _(i):
            at = pl.multiple_of(EX * i, 8)
            c_own = R[s, 0, pl.ds(at + 8, NB), :]
            FX[s, i + 1, :, :] = 0.5 * (c_own + R[s, 0, pl.ds(at + EX + 8, NB), :])
            FY[s, i, 0:NB, :] = 0.5 * (c_own + R[s, 0, pl.ds(at + 7, NB), :])

    @pl.loop(0, 57)
    def _(i):
        for s in range(2):
            for h in range(2):
                R[s, h, pl.ds(pl.multiple_of(EX * i, 8), EX), :] = jnp.zeros((EX, LANES), F32)

    when_all(has_side, lambda d: c_recv(d).wait_recv())
    for s in range(2):
        for d in range(4):
            own = ces[d, s]
            face = jnp.where(has_side[d], 0.5 * (own + cer[d, s]), own)
            if d == 0:
                FX[s, 0, :, :] = face
            elif d == 1:
                FX[s, NB, :, :] = face
            elif d == 2:
                FY[s, :, 0, :] = face
            else:
                FY[s, :, NB, :] = face
            FE[s, d] = face
    for s in range(2):
        for h in range(2):
            f_copy(s, h).wait()
        stencil(s, None, True)
        wait_z(s, ROWS + COLS)
        edge_fix(s, 1.0, ROWS + COLS)
        send_early(s, 0, False)
        send_late(s, 0, False)

    for s in range(2):
        for cp in s_copies(s, True):
            cp.wait()
        inner_product(s)
    for s in range(2):
        for cp in s_copies(s, False):
            cp.wait()

    def early(s, p):
        wait_z(s, ROWS)
        edge_fix(s, om_ref[s], ROWS)
        send_early(s, p, True)

    def late(s, p):
        wait_z(s, COLS)
        edge_fix(s, om_ref[s], COLS)
        send_late(s, p, True)

    def half_sweep(s, p, other, p_other, started):
        @pl.when(started)
        def _():
            early(other, p_other)
        wait_frames(s, p)
        scatter_frames(s, p)
        fill_frame(s)
        for m in range(CHUNKS):
            z = frame_product(s, m)
            for h in range(2):
                Z[s, h, pl.ds(1 + m * g, g), 8:EX, :] = z[h]
            if m == LATE_AT:
                @pl.when(started)
                def _():
                    late(other, p_other)
        send_z_edges(s, True)

    @pl.loop(0, SWEEPS - 1)
    def _(k):
        p = lax.rem(k, 2)
        half_sweep(0, p, 1, p, k > 0)

        @pl.when(k > 0)
        def _():
            inner_product(1, 0)

        @pl.when(k == 0)
        def _():
            stencil(0, om_ref[0], False)
        half_sweep(1, p, 0, 1 - p, k >= 0)
        inner_product(0, 1)

    last = (SWEEPS - 1) % 2

    def finish(s, m):
        z = frame_product(s, m)
        for h in range(2):
            U[s, h, pl.ds(m * g, g)] = U[s, h, pl.ds(m * g, g)] + om_ref[s] * z[h]

    def write_out(s):
        for h in range(2):
            for m in range(CHUNKS):
                o_copy(s, h, m).start()

    early(1, last)
    wait_frames(0, last)
    scatter_frames(0, last)
    fill_frame(0)
    for m in range(CHUNKS):
        finish(0, m)
        if m == LATE_AT:
            late(1, last)
    write_out(0)
    inner_product(1)
    wait_frames(1, last)
    scatter_frames(1, last)
    fill_frame(1)
    for m in range(CHUNKS):
        finish(1, m)
    write_out(1)
    when_all(has_side, lambda d: c_send(d).wait_send())
    for s in range(2):
        when_all(has_side, lambda d: z_send(s, d).wait_send())
        when_all(has_side, lambda d: e_copy(s, d, OPP_SIDE[d], last).wait_send(), COLS)
        when_all(has_side, lambda d: f_copy_remote(s, d, OPP_SIDE[d], last).wait_send())
        when_all(has_corner, lambda q: k_copy(s, q, 3 - q, last).wait_send())
        for h in range(2):
            for m in range(CHUNKS):
                o_copy(s, h, m).wait()


def solution(mesh):
    grid_spec = P(None, "row", "col", None)

    def local(forcing, init_guess, cell_coef, solve_rows, relax_factor):
        num_sys, nb, _, rhs = forcing.shape
        s_mat = jnp.swapaxes(solve_rows, 3, 4).reshape(num_sys, EX // 2, 7, 16, nb * nb)
        any_spec = pl.BlockSpec(memory_space=pl.ANY)
        dma = pltpu.SemaphoreType.DMA
        return pl.pallas_call(
            kernel,
            name="schwarz",
            out_shape=jax.ShapeDtypeStruct(forcing.shape, F32),
            in_specs=[any_spec, any_spec, pl.BlockSpec(memory_space=pltpu.VMEM), any_spec, pl.BlockSpec(memory_space=pltpu.SMEM)],
            out_specs=any_spec,
            scratch_shapes=[
                pltpu.VMEM((2, 24, 4, 16, NB * NB), BF16),
                pltpu.VMEM((2, 4, 7, 16, NB * NB), BF16),
                pltpu.VMEM((2, 24, 3, 16, NB * NB), BF16),
                pltpu.VMEM((2, 2, 50, 64, LANES), F32),
                pltpu.VMEM((2, 2, 57 * EX, LANES), F32),
                pltpu.VMEM((2, EX * EX, 2 * LANES), BF16),
                pltpu.VMEM((2, 2, NB, NB, LANES), F32),
                pltpu.VMEM((2, NB + 1, NB, LANES), F32),
                pltpu.VMEM((2, NB, EX, LANES), F32),
                pltpu.VMEM((2, 4, NB, LANES), F32),
                pltpu.VMEM((4, 2, NB, LANES), F32),
                pltpu.VMEM((4, 2, NB, LANES), F32),
                pltpu.VMEM((2, 4, 2, NB, LANES), F32),
                pltpu.VMEM((2, 4, 2, NB, LANES), F32),
                pltpu.VMEM((2, 4, MG, NB, 2 * LANES), BF16),
                pltpu.VMEM((2, 2, 4, MG, NB, 2 * LANES), BF16),
                pltpu.VMEM((2, 4, 32, 2 * LANES), BF16),
                pltpu.VMEM((2, 2, 4, 32, 2 * LANES), BF16),
                dma((2, 2)), dma((2, 2)), dma((2, 7)), dma((2, 2, CHUNKS)),
                dma((4,)), dma((4,)), dma((2, 4)), dma((2, 4)),
                dma((2, 4)), dma((2, 2, 4)), dma((2, 4)), dma((2, 2, 4)), dma((2, 4)), dma((2, 2, 4)),
            ],
            compiler_params=pltpu.CompilerParams(collective_id=0, has_side_effects=True, vmem_limit_bytes=66_000_000),
            cost_estimate=pl.CostEstimate(flops=30_000_000_000, bytes_accessed=43_000_000, transcendentals=0),
        )(forcing, init_guess, cell_coef, s_mat, relax_factor)

    return jax.shard_map(local, mesh=mesh, in_specs=(grid_spec, grid_spec, P(None, "row", "col"), P(None, "row", "col", None, None), P(None)), out_specs=grid_spec, check_vma=False)
```

```python
import jax
import jax.numpy as jnp
from jax import lax
from jax.experimental import pallas as pl
from jax.experimental.pallas import tpu as pltpu
from jax.sharding import PartitionSpec as P

SWEEPS = 4
MESH_ID = pl.DeviceIdType.MESH
NB = 48
MG = 4
EX = NB + 2 * MG
LANES = 128
CHUNKS = 3
LATE_AT = 2
OFF = 4
KI = 24 * 64
KF = EX * EX - KI
SIDES = ((-1, 0), (1, 0), (0, -1), (0, 1))
OPP_SIDE = (1, 0, 3, 2)
CORNERS = ((-1, -1), (-1, 1), (1, -1), (1, 1))
F32 = jnp.float32
BF16 = jnp.bfloat16


def kernel(f_hbm, u_hbm, c_hbm, s_hbm, om_ref, U,
           c_ref, SI, SA, SF, Z, R, W, FX, FY, FE, ces, cer, zes, zer, frs, frr, crs, crr,
           sem_c, sem_f, sem_u, sem_s, sem_cs, sem_cr, sem_zs, sem_zr,
           sem_fs, sem_fr, sem_ks, sem_kr, sem_es, sem_er):
    row = lax.axis_index("row")
    col = lax.axis_index("col")
    has_side = (row > 0, row < 3, col > 0, col < 3)
    has_corner = tuple(
        jnp.logical_and(has_side[0] if dr < 0 else has_side[1], has_side[2] if dc < 0 else has_side[3])
        for dr, dc in CORNERS)

    def dev(delta):
        return {"row": row + delta[0], "col": col + delta[1]}

    def ext_col(j):
        return pl.ds(OFF + EX * MG + j, NB, stride=EX)

    def own_row(i):
        start = OFF + EX * (MG + i) + MG
        return pl.ds(start if isinstance(i, int) else pl.multiple_of(start, 8), NB)

    def u_copy(s, h):
        return pltpu.make_async_copy(u_hbm.at[s, :, :, pl.ds(h * LANES, LANES)], Z.at[s, h, pl.ds(1, NB), pl.ds(8, NB), :], sem_u.at[s, h])

    def f_copy(s, h):
        return pltpu.make_async_copy(f_hbm.at[s, :, :, pl.ds(h * LANES, LANES)], U.at[s, h], sem_f.at[s, h])

    rows_per = NB * NB // CHUNKS

    mid = pl.ds(2, 24)

    def s_copies(s, inner):
        parts = (
            (s_hbm.at[s, mid, pl.ds(1, 2)], SI.at[s, :, pl.ds(0, 2)]),
            (s_hbm.at[s, mid, pl.ds(4, 2)], SI.at[s, :, pl.ds(2, 2)]),
            (s_hbm.at[s, pl.ds(0, 2)], SA.at[s, pl.ds(0, 2)]),
            (s_hbm.at[s, pl.ds(26, 2)], SA.at[s, pl.ds(2, 2)]),
            (s_hbm.at[s, mid, pl.ds(0, 1)], SF.at[s, :, pl.ds(0, 1)]),
            (s_hbm.at[s, mid, pl.ds(3, 1)], SF.at[s, :, pl.ds(1, 1)]),
            (s_hbm.at[s, mid, pl.ds(6, 1)], SF.at[s, :, pl.ds(2, 1)]))
        return [pltpu.make_async_copy(src, dst, sem_s.at[s, m]) for m, (src, dst) in enumerate(parts) if (m < 2) == inner]

    c_copy = pltpu.make_async_copy(c_hbm, c_ref, sem_c)
    c_copy.start()
    for s in range(2):
        for h in range(2):
            u_copy(s, h).start()
    for s in range(2):
        for h in range(2):
            f_copy(s, h).start()

    barrier = pltpu.get_barrier_semaphore()
    n_side = sum(h.astype(jnp.int32) for h in has_side) + sum(h.astype(jnp.int32) for h in has_corner)
    for cond, delta in zip(has_side + has_corner, SIDES + CORNERS):
        @pl.when(cond)
        def _(delta=delta):
            pl.semaphore_signal(barrier, inc=1, device_id=dev(delta), device_id_type=MESH_ID)

    c_copy.wait()
    for s in range(2):
        c_t = c_ref[s].T
        for i in range(NB):
            R[s, 0, pl.ds(EX * i + 8, NB), :] = jnp.broadcast_to(c_t[:, i:i + 1], (NB, LANES))

    zero_row = jnp.zeros((64, LANES), F32)

    def zero_z(s, h):
        Z[s, h, 0, :, :] = zero_row
        Z[s, h, 49, :, :] = zero_row

        @pl.loop(1, 49)
        def _(i):
            Z[s, h, i, 0:8, :] = jnp.zeros((8, LANES), F32)
            Z[s, h, i, EX:64, :] = jnp.zeros((8, LANES), F32)

    for s in range(2):
        for h in range(2):
            zero_z(s, h)

    for d in range(4):
        @pl.when(jnp.logical_not(has_side[d]))
        def _(d=d):
            for s in range(2):
                zer[s, d] = jnp.zeros((2, NB, LANES), F32)
                cer[d, s] = jnp.zeros((NB, LANES), F32)
                for p in range(2):
                    frr[p, s, d] = jnp.zeros((MG, NB, 2 * LANES), BF16)
    for q in range(4):
        @pl.when(jnp.logical_not(has_corner[q]))
        def _(q=q):
            for s in range(2):
                for p in range(2):
                    crr[p, s, q] = jnp.zeros((32, 2 * LANES), BF16)

    for s in range(2):
        ces[0, s] = R[s, 0, pl.ds(8, NB), :]
        ces[1, s] = R[s, 0, pl.ds(EX * (NB - 1) + 8, NB), :]
        ces[2, s] = R[s, 0, pl.ds(8, NB, stride=EX), :]
        ces[3, s] = R[s, 0, pl.ds(EX - 1, NB, stride=EX), :]

    pl.semaphore_wait(barrier, n_side)

    def c_send(d):
        return pltpu.make_async_remote_copy(ces.at[d], cer.at[OPP_SIDE[d]], sem_cs.at[d], sem_cr.at[OPP_SIDE[d]], device_id=dev(SIDES[d]), device_id_type=MESH_ID)

    def c_recv(d):
        return pltpu.make_async_remote_copy(ces.at[OPP_SIDE[d]], cer.at[d], sem_cs.at[OPP_SIDE[d]], sem_cr.at[d], device_id=dev(SIDES[d]), device_id_type=MESH_ID)

    for d in range(4):
        @pl.when(has_side[d])
        def _(d=d):
            c_send(d).start()

    def remote(src, dst, ssem, rsem, delta):
        return pltpu.make_async_remote_copy(src, dst, ssem, rsem, device_id=dev(delta), device_id_type=MESH_ID)

    def z_copy(s, d, slot):
        return remote(zes.at[s, d], zer.at[s, slot], sem_zs.at[s, d], sem_zr.at[s, slot], SIDES[d])

    def z_send(s, d):
        return z_copy(s, d, OPP_SIDE[d])

    def z_recv(s, d):
        return z_copy(s, OPP_SIDE[d], d)

    def early_layers(d):
        return pl.ds(1, 3) if d == 2 else pl.ds(0, 3)

    def late_layers(d):
        return (pl.ds(0, 4), pl.ds(0, 4), pl.ds(0, 1), pl.ds(3, 1))[d]

    def e_copy(s, d, slot, p):
        lay = early_layers(d)
        return remote(frs.at[s, d, lay], frr.at[p, s, slot, lay], sem_es.at[s, d], sem_er.at[p, s, slot], SIDES[d])

    def f_copy_remote(s, d, slot, p):
        lay = late_layers(d)
        return remote(frs.at[s, d, lay], frr.at[p, s, slot, lay], sem_fs.at[s, d], sem_fr.at[p, s, slot], SIDES[d])

    def k_copy(s, q, slot, p):
        return remote(crs.at[s, q], crr.at[p, s, slot], sem_ks.at[s, q], sem_kr.at[p, s, slot], CORNERS[q])

    def when_all(conds, body, order=None):
        for i in (order or range(len(conds))):
            @pl.when(conds[i])
            def _(i=i):
                body(i)

    COLS = (2, 3)
    ROWS = (0, 1)

    def send_z_edges(s, again):
        if again:
            when_all(has_side, lambda d: z_send(s, d).wait_send())
        for h in range(2):
            zes[s, 2, h] = Z[s, h, 1:NB + 1, 8, :]
            zes[s, 3, h] = Z[s, h, 1:NB + 1, EX - 1, :]
        for h in range(2):
            zes[s, 0, h] = Z[s, h, 1, 8:EX, :]
            zes[s, 1, h] = Z[s, h, NB, 8:EX, :]
        when_all(has_side, lambda d: z_send(s, d).start(), COLS + ROWS)

    def stencil(s, om, first):
        @pl.loop(0, NB)
        def _(i):
            ax0 = FX[s, i, :, :]
            ax1 = FX[s, i + 1, :, :]
            ay0 = FY[s, i, 0:NB, :]
            ay1 = FY[s, i, 1:NB + 1, :]
            for h in range(2):
                zc = Z[s, h, i + 1, 8:EX, :]
                zl = Z[s, h, i + 1, 7:EX - 1, :]
                zr = Z[s, h, i + 1, 9:EX + 1, :]
                zu = Z[s, h, i, 8:EX, :]
                zd = Z[s, h, i + 2, 8:EX, :]
                av = ax0 * (zc - zu) - ax1 * (zd - zc) + ay0 * (zc - zl) - ay1 * (zr - zc)
                if first:
                    R[s, h, own_row(i), :] = U[s, h, i] - av
                    U[s, h, i] = zc
                else:
                    R[s, h, own_row(i), :] = R[s, h, own_row(i), :] - om * av
                    U[s, h, i] = U[s, h, i] + om * zc

    def stencil_rows(s, om, rows):
        for h in range(2):
            zc = Z[s, h, rows[0] + 1, 8:EX, :]
            flux = FX[s, rows[0], :, :] * (zc - Z[s, h, rows[0], 8:EX, :])
            for i in rows:
                zd = Z[s, h, i + 2, 8:EX, :]
                down = FX[s, i + 1, :, :] * (zd - zc)
                side = FY[s, i, 0:NB, :] * (zc - Z[s, h, i + 1, 7:EX - 1, :]) - FY[s, i, 1:NB + 1, :] * (Z[s, h, i + 1, 9:EX + 1, :] - zc)
                R[s, h, own_row(i), :] = R[s, h, own_row(i), :] - om * ((flux - down) + side)
                U[s, h, i] = U[s, h, i] + om * zc
                flux, zc = down, zd

    def wait_z(s, sides):
        when_all(has_side, lambda d: z_recv(s, d).wait_recv(), sides)

    def edge_fix(s, om, sides):
        for d in sides:
            for h in range(2):
                cells = (own_row(0), own_row(NB - 1), ext_col(MG), ext_col(MG + NB - 1))[d]
                R[s, h, cells, :] = R[s, h, cells, :] + om * (FE[s, d] * (zer[s, d, h] - zes[s, d, h]))

    def pack_col(s, h, d, a):
        first = MG if d == 2 else NB
        frs[s, d, a, :, pl.ds(h * LANES, LANES)] = R[s, h, ext_col(first + a), :].astype(BF16)

    def send_early(s, p, again):
        if again:
            when_all(has_side, lambda d: e_copy(s, d, OPP_SIDE[d], p).wait_send(), COLS)
        for d in COLS:
            for h in range(2):
                for a in ((1, 2, 3) if d == 2 else (0, 1, 2)):
                    pack_col(s, h, d, a)
        when_all(has_side, lambda d: e_copy(s, d, OPP_SIDE[d], p).start(), COLS)

    def send_late(s, p, again):
        if again:
            when_all(has_side, lambda d: f_copy_remote(s, d, OPP_SIDE[d], p).wait_send())
            when_all(has_corner, lambda q: k_copy(s, q, 3 - q, p).wait_send())
        for h in range(2):
            lanes = pl.ds(h * LANES, LANES)
            pack_col(s, h, 2, 0)
            pack_col(s, h, 3, 3)
            for a in range(MG):
                frs[s, 0, a, :, lanes] = R[s, h, own_row(a), :].astype(BF16)
                frs[s, 1, a, :, lanes] = R[s, h, own_row(NB - MG + a), :].astype(BF16)
            for q, (dr, dc) in enumerate(CORNERS):
                r0 = MG if dr < 0 else NB
                c0 = 0 if dc < 0 else NB
                tile = [R[s, h, pl.ds(OFF + EX * (r0 + a) + c0, 8), :] for a in range(MG)]
                crs[s, q, :, lanes] = jnp.concatenate(tile, axis=0).astype(BF16)
        when_all(has_side, lambda d: f_copy_remote(s, d, OPP_SIDE[d], p).start(), COLS + ROWS)
        when_all(has_corner, lambda q: k_copy(s, q, 3 - q, p).start())

    def wait_frames(s, p):
        when_all(has_side, lambda d: e_copy(s, OPP_SIDE[d], d, p).wait_recv(), COLS)
        when_all(has_side, lambda d: f_copy_remote(s, OPP_SIDE[d], d, p).wait_recv())
        when_all(has_corner, lambda q: k_copy(s, 3 - q, q, p).wait_recv())

    def scatter_frames(s, p):
        for d in range(4):
            for h in range(2):
                for a in range(MG):
                    cells = (own_row(a - MG), own_row(NB + a), ext_col(a), ext_col(MG + NB + a))[d]
                    R[s, h, cells, :] = frr[p, s, d, a, :, pl.ds(h * LANES, LANES)].astype(F32)
        for q, (dr, dc) in enumerate(CORNERS):
            r0 = 0 if dr < 0 else MG + NB
            for h in range(2):
                v = crr[p, s, q, :, pl.ds(h * LANES, LANES)].astype(F32)
                for a in range(MG):
                    if dc < 0:
                        R[s, h, pl.ds(OFF + EX * (r0 + a), 4), :] = v[8 * a:8 * a + 4]
                    else:
                        R[s, h, pl.ds(OFF + EX * (r0 + a) + MG + NB, 4), :] = v[8 * a + 4:8 * a + 8]

    def pair_rows(s, h, t):
        return R[s, h, pl.ds(2 * EX * t + OFF, 2 * EX), :].astype(BF16)

    def fill(s, t, tile, n, base):
        for h in range(2):
            v = R[s, h, pl.ds(2 * EX * t + 16 * tile + OFF, 16 * n), :].astype(BF16)
            W[s, pl.ds(base, 16 * n), pl.ds(h * LANES, LANES)] = v

    def fill_inner(s):
        for t in range(2, 26):
            fill(s, t, 1, 2, 64 * (t - 2))
            fill(s, t, 4, 2, 64 * (t - 2) + 32)

    def fill_frame(s):
        fill(s, 0, 0, 14, KI)
        fill(s, 26, 0, 14, KI + 224)
        for t in range(2, 26):
            for n, u in enumerate((0, 3, 6)):
                fill(s, t, u, 1, KI + 448 + 48 * (t - 2) + 16 * n)

    g = NB // CHUNKS

    def matmul(s, m, parts, k0):
        cells = pl.ds(m * rows_per, rows_per)
        lhs = [p[s, :, :, :, cells].reshape(-1, rows_per) for p in parts]
        lhs = jnp.concatenate(lhs, axis=0) if len(lhs) > 1 else lhs[0]
        z = lax.dot_general(lhs, W[s, pl.ds(k0, lhs.shape[0]), :], (((0,), (0,)), ((), ())), preferred_element_type=F32)
        return z.reshape(g, NB, 2 * LANES)

    def inner_product(s, other=None):
        fill_inner(s)
        for m in range(CHUNKS):
            if other is not None:
                stencil_rows(other, om_ref[other], range(m * g, (m + 1) * g))
            z = matmul(s, m, (SI,), 0)
            for h in range(2):
                Z[s, h, pl.ds(1 + m * g, g), 8:EX, :] = z[:, :, h * LANES:(h + 1) * LANES]

    def frame_product(s, m):
        z = matmul(s, m, (SA, SF), KI)
        return [Z[s, h, pl.ds(1 + m * g, g), 8:EX, :] + z[:, :, h * LANES:(h + 1) * LANES] for h in range(2)]

    for s in range(2):
        for h in range(2):
            u_copy(s, h).wait()
        send_z_edges(s, False)
    for first in (True, False):
        for s in range(2):
            for cp in s_copies(s, first):
                cp.start()
    for s in range(2):
        for i in range(NB):
            R[s, 0, pl.ds(EX * i, 8), :] = jnp.zeros((8, LANES), F32)

        @pl.loop(0, NB)
        def _(i):
            at = pl.multiple_of(EX * i, 8)
            c_own = R[s, 0, pl.ds(at + 8, NB), :]
            FX[s, i + 1, :, :] = 0.5 * (c_own + R[s, 0, pl.ds(at + EX + 8, NB), :])
            FY[s, i, 0:NB, :] = 0.5 * (c_own + R[s, 0, pl.ds(at + 7, NB), :])

    for s in range(2):
        for d in range(4):
            face = jnp.where(has_side[d], 0.0, ces[d, s])
            if d == 0:
                FX[s, 0, :, :] = face
            elif d == 1:
                FX[s, NB, :, :] = face
            elif d == 2:
                FY[s, :, 0, :] = face
            else:
                FY[s, :, NB, :] = face

    @pl.loop(0, 57)
    def _(i):
        for s in range(2):
            for h in range(2):
                R[s, h, pl.ds(pl.multiple_of(EX * i, 8), EX), :] = jnp.zeros((EX, LANES), F32)

    for s in range(2):
        for h in range(2):
            f_copy(s, h).wait()
        stencil(s, None, True)
    when_all(has_side, lambda d: c_recv(d).wait_recv())
    for s in range(2):
        for d in range(4):
            FE[s, d] = jnp.where(has_side[d], 0.5 * (ces[d, s] + cer[d, s]), 0.0)
    for s in range(2):
        wait_z(s, ROWS + COLS)
        edge_fix(s, 1.0, ROWS + COLS)
        send_early(s, 0, False)
        send_late(s, 0, False)

    for s in range(2):
        for cp in s_copies(s, True):
            cp.wait()
        inner_product(s)
    for s in range(2):
        for cp in s_copies(s, False):
            cp.wait()

    def early(s, p):
        wait_z(s, ROWS)
        edge_fix(s, om_ref[s], ROWS)
        send_early(s, p, True)

    def late(s, p):
        wait_z(s, COLS)
        edge_fix(s, om_ref[s], COLS)
        send_late(s, p, True)

    def half_sweep(s, p, other, p_other, started):
        @pl.when(started)
        def _():
            early(other, p_other)
        wait_frames(s, p)
        scatter_frames(s, p)
        fill_frame(s)
        for m in range(CHUNKS):
            z = frame_product(s, m)
            for h in range(2):
                Z[s, h, pl.ds(1 + m * g, g), 8:EX, :] = z[h]
            if m == LATE_AT:
                @pl.when(started)
                def _():
                    late(other, p_other)
        send_z_edges(s, True)

    @pl.loop(0, SWEEPS - 1)
    def _(k):
        p = lax.rem(k, 2)
        half_sweep(0, p, 1, p, k > 0)

        @pl.when(k > 0)
        def _():
            inner_product(1, 0)

        @pl.when(k == 0)
        def _():
            stencil(0, om_ref[0], False)
        half_sweep(1, p, 0, 1 - p, k >= 0)
        inner_product(0, 1)

    last = (SWEEPS - 1) % 2

    def finish(s, m):
        z = frame_product(s, m)
        for h in range(2):
            U[s, h, pl.ds(m * g, g)] = U[s, h, pl.ds(m * g, g)] + om_ref[s] * z[h]

    early(1, last)
    wait_frames(0, last)
    scatter_frames(0, last)
    fill_frame(0)
    for m in range(CHUNKS):
        finish(0, m)
        if m == LATE_AT:
            late(1, last)
    inner_product(1)
    wait_frames(1, last)
    scatter_frames(1, last)
    fill_frame(1)
    for m in range(CHUNKS):
        finish(1, m)
    when_all(has_side, lambda d: c_send(d).wait_send())
    for s in range(2):
        when_all(has_side, lambda d: z_send(s, d).wait_send())
        when_all(has_side, lambda d: e_copy(s, d, OPP_SIDE[d], last).wait_send(), COLS)
        when_all(has_side, lambda d: f_copy_remote(s, d, OPP_SIDE[d], last).wait_send())
        when_all(has_corner, lambda q: k_copy(s, q, 3 - q, last).wait_send())


def write_out(u_ref, out_hbm, sem):
    def copy(s, h, m):
        g = NB // CHUNKS
        return pltpu.make_async_copy(u_ref.at[s, h, pl.ds(m * g, g)], out_hbm.at[s, pl.ds(m * g, g), :, pl.ds(h * LANES, LANES)], sem.at[s, h, m])
    for act in ("start", "wait"):
        for s in range(2):
            for h in range(2):
                for m in range(CHUNKS):
                    getattr(copy(s, h, m), act)()


def solution(mesh):
    grid_spec = P(None, "row", "col", None)

    def local(forcing, init_guess, cell_coef, solve_rows, relax_factor):
        num_sys, nb, _, rhs = forcing.shape
        s_mat = jnp.swapaxes(solve_rows, 3, 4).reshape(num_sys, EX // 2, 7, 16, nb * nb)
        any_spec = pl.BlockSpec(memory_space=pl.ANY)
        dma = pltpu.SemaphoreType.DMA
        approx = pl.pallas_call(
            kernel,
            name="schwarz",
            out_shape=pltpu.VMEM((2, 2, NB, NB, LANES), F32),
            in_specs=[any_spec, any_spec, any_spec, any_spec, pl.BlockSpec(memory_space=pltpu.SMEM)],
            out_specs=pl.BlockSpec(memory_space=pltpu.VMEM),
            scratch_shapes=[
                pltpu.VMEM((2, NB, NB), F32),
                pltpu.VMEM((2, 24, 4, 16, NB * NB), BF16),
                pltpu.VMEM((2, 4, 7, 16, NB * NB), BF16),
                pltpu.VMEM((2, 24, 3, 16, NB * NB), BF16),
                pltpu.VMEM((2, 2, 50, 64, LANES), F32),
                pltpu.VMEM((2, 2, 57 * EX, LANES), F32),
                pltpu.VMEM((2, EX * EX, 2 * LANES), BF16),
                pltpu.VMEM((2, NB + 1, NB, LANES), F32),
                pltpu.VMEM((2, NB, EX, LANES), F32),
                pltpu.VMEM((2, 4, NB, LANES), F32),
                pltpu.VMEM((4, 2, NB, LANES), F32),
                pltpu.VMEM((4, 2, NB, LANES), F32),
                pltpu.VMEM((2, 4, 2, NB, LANES), F32),
                pltpu.VMEM((2, 4, 2, NB, LANES), F32),
                pltpu.VMEM((2, 4, MG, NB, 2 * LANES), BF16),
                pltpu.VMEM((2, 2, 4, MG, NB, 2 * LANES), BF16),
                pltpu.VMEM((2, 4, 32, 2 * LANES), BF16),
                pltpu.VMEM((2, 2, 4, 32, 2 * LANES), BF16),
                dma, dma((2, 2)), dma((2, 2)), dma((2, 7)),
                dma((4,)), dma((4,)), dma((2, 4)), dma((2, 4)),
                dma((2, 4)), dma((2, 2, 4)), dma((2, 4)), dma((2, 2, 4)), dma((2, 4)), dma((2, 2, 4)),
            ],
            compiler_params=pltpu.CompilerParams(collective_id=0, has_side_effects=True, vmem_limit_bytes=61_500_000),
            cost_estimate=pl.CostEstimate(flops=30_000_000_000, bytes_accessed=43_000_000, transcendentals=0),
        )(forcing, init_guess, cell_coef, s_mat, relax_factor)
        return pl.pallas_call(
            write_out,
            name="write_out",
            out_shape=jax.ShapeDtypeStruct(forcing.shape, F32),
            in_specs=[pl.BlockSpec(memory_space=pltpu.VMEM)],
            out_specs=any_spec,
            scratch_shapes=[dma((2, 2, CHUNKS))],
            compiler_params=pltpu.CompilerParams(vmem_limit_bytes=8_000_000),
            cost_estimate=pl.CostEstimate(flops=1_000_000, bytes_accessed=9_500_000, transcendentals=0),
        )(approx)

    return jax.shard_map(local, mesh=mesh, in_specs=(grid_spec, grid_spec, P(None, "row", "col"), P(None, "row", "col", None, None), P(None)), out_specs=grid_spec, check_vma=False)
```

```python
import jax
import jax.numpy as jnp
from jax import lax
from jax.experimental import pallas as pl
from jax.experimental.pallas import tpu as pltpu
from jax.sharding import PartitionSpec as P

SWEEPS = 4
MESH_ID = pl.DeviceIdType.MESH
NB = 48
MG = 4
EX = NB + 2 * MG
LANES = 128
CHUNKS = 3
LATE_AT = 2
OFF = 4
KI = 24 * 64
KF = EX * EX - KI
SIDES = ((-1, 0), (1, 0), (0, -1), (0, 1))
OPP_SIDE = (1, 0, 3, 2)
CORNERS = ((-1, -1), (-1, 1), (1, -1), (1, 1))
F32 = jnp.float32
BF16 = jnp.bfloat16


def kernel(f_hbm, u_hbm, c_hbm, s_hbm, om_ref, U,
           c_ref, SI, SA, SF, Z, R, W, FX, FY, FE, ces, cer, zes, zer, frs, frr, crs, crr,
           sem_c, sem_f, sem_u, sem_s, sem_cs, sem_cr, sem_zs, sem_zr,
           sem_fs, sem_fr, sem_ks, sem_kr, sem_es, sem_er):
    row = lax.axis_index("row")
    col = lax.axis_index("col")
    has_side = (row > 0, row < 3, col > 0, col < 3)
    has_corner = tuple(
        jnp.logical_and(has_side[0] if dr < 0 else has_side[1], has_side[2] if dc < 0 else has_side[3])
        for dr, dc in CORNERS)

    def dev(delta):
        return {"row": row + delta[0], "col": col + delta[1]}

    def ext_col(j):
        return pl.ds(OFF + EX * MG + j, NB, stride=EX)

    def own_row(i):
        start = OFF + EX * (MG + i) + MG
        return pl.ds(start if isinstance(i, int) else pl.multiple_of(start, 8), NB)

    def u_copy(s, h):
        return pltpu.make_async_copy(u_hbm.at[s, :, :, pl.ds(h * LANES, LANES)], Z.at[s, h, pl.ds(1, NB), pl.ds(8, NB), :], sem_u.at[s, h])

    def f_copy(s, h):
        return pltpu.make_async_copy(f_hbm.at[s, :, :, pl.ds(h * LANES, LANES)], U.at[s, h], sem_f.at[s, h])

    rows_per = NB * NB // CHUNKS

    mid = pl.ds(2, 24)

    def s_copies(s, inner):
        parts = (
            (s_hbm.at[s, mid, pl.ds(1, 2)], SI.at[s, :, pl.ds(0, 2)]),
            (s_hbm.at[s, mid, pl.ds(4, 2)], SI.at[s, :, pl.ds(2, 2)]),
            (s_hbm.at[s, pl.ds(0, 2)], SA.at[s, pl.ds(0, 2)]),
            (s_hbm.at[s, pl.ds(26, 2)], SA.at[s, pl.ds(2, 2)]),
            (s_hbm.at[s, mid, pl.ds(0, 1)], SF.at[s, :, pl.ds(0, 1)]),
            (s_hbm.at[s, mid, pl.ds(3, 1)], SF.at[s, :, pl.ds(1, 1)]),
            (s_hbm.at[s, mid, pl.ds(6, 1)], SF.at[s, :, pl.ds(2, 1)]))
        return [pltpu.make_async_copy(src, dst, sem_s.at[s, m]) for m, (src, dst) in enumerate(parts) if (m < 2) == inner]

    c_copy = pltpu.make_async_copy(c_hbm, c_ref, sem_c)
    c_copy.start()
    for s in range(2):
        for h in range(2):
            u_copy(s, h).start()
    for s in range(2):
        for h in range(2):
            f_copy(s, h).start()

    barrier = pltpu.get_barrier_semaphore()
    n_side = sum(h.astype(jnp.int32) for h in has_side) + sum(h.astype(jnp.int32) for h in has_corner)
    for cond, delta in zip(has_side + has_corner, SIDES + CORNERS):
        @pl.when(cond)
        def _(delta=delta):
            pl.semaphore_signal(barrier, inc=1, device_id=dev(delta), device_id_type=MESH_ID)

    c_copy.wait()
    for s in range(2):
        c_t = c_ref[s].T
        for i in range(NB):
            R[s, 0, pl.ds(EX * i + 8, NB), :] = jnp.broadcast_to(c_t[:, i:i + 1], (NB, LANES))

    zero_row = jnp.zeros((64, LANES), F32)

    def zero_z(s, h):
        Z[s, h, 0, :, :] = zero_row
        Z[s, h, 49, :, :] = zero_row

        @pl.loop(1, 49)
        def _(i):
            Z[s, h, i, 0:8, :] = jnp.zeros((8, LANES), F32)
            Z[s, h, i, EX:64, :] = jnp.zeros((8, LANES), F32)

    for s in range(2):
        for h in range(2):
            zero_z(s, h)

    for d in range(4):
        @pl.when(jnp.logical_not(has_side[d]))
        def _(d=d):
            for s in range(2):
                zer[s, d] = jnp.zeros((2, NB, LANES), F32)
                cer[d, s] = jnp.zeros((NB, LANES), F32)
                for p in range(2):
                    frr[p, s, d] = jnp.zeros((MG, NB, 2 * LANES), BF16)
    for q in range(4):
        @pl.when(jnp.logical_not(has_corner[q]))
        def _(q=q):
            for s in range(2):
                for p in range(2):
                    crr[p, s, q] = jnp.zeros((32, 2 * LANES), BF16)

    for s in range(2):
        ces[0, s] = R[s, 0, pl.ds(8, NB), :]
        ces[1, s] = R[s, 0, pl.ds(EX * (NB - 1) + 8, NB), :]
        ces[2, s] = R[s, 0, pl.ds(8, NB, stride=EX), :]
        ces[3, s] = R[s, 0, pl.ds(EX - 1, NB, stride=EX), :]

    pl.semaphore_wait(barrier, n_side)

    def c_send(d):
        return pltpu.make_async_remote_copy(ces.at[d], cer.at[OPP_SIDE[d]], sem_cs.at[d], sem_cr.at[OPP_SIDE[d]], device_id=dev(SIDES[d]), device_id_type=MESH_ID)

    def c_recv(d):
        return pltpu.make_async_remote_copy(ces.at[OPP_SIDE[d]], cer.at[d], sem_cs.at[OPP_SIDE[d]], sem_cr.at[d], device_id=dev(SIDES[d]), device_id_type=MESH_ID)

    for d in range(4):
        @pl.when(has_side[d])
        def _(d=d):
            c_send(d).start()

    def remote(src, dst, ssem, rsem, delta):
        return pltpu.make_async_remote_copy(src, dst, ssem, rsem, device_id=dev(delta), device_id_type=MESH_ID)

    def z_copy(s, d, slot):
        return remote(zes.at[s, d], zer.at[s, slot], sem_zs.at[s, d], sem_zr.at[s, slot], SIDES[d])

    def z_send(s, d):
        return z_copy(s, d, OPP_SIDE[d])

    def z_recv(s, d):
        return z_copy(s, OPP_SIDE[d], d)

    def early_layers(d):
        return pl.ds(1, 3) if d == 2 else pl.ds(0, 3)

    def late_layers(d):
        return (pl.ds(0, 4), pl.ds(0, 4), pl.ds(0, 1), pl.ds(3, 1))[d]

    def e_copy(s, d, slot, p):
        lay = early_layers(d)
        return remote(frs.at[s, d, lay], frr.at[p, s, slot, lay], sem_es.at[s, d], sem_er.at[p, s, slot], SIDES[d])

    def f_copy_remote(s, d, slot, p):
        lay = late_layers(d)
        return remote(frs.at[s, d, lay], frr.at[p, s, slot, lay], sem_fs.at[s, d], sem_fr.at[p, s, slot], SIDES[d])

    def k_copy(s, q, slot, p):
        return remote(crs.at[s, q], crr.at[p, s, slot], sem_ks.at[s, q], sem_kr.at[p, s, slot], CORNERS[q])

    def when_all(conds, body, order=None):
        for i in (order or range(len(conds))):
            @pl.when(conds[i])
            def _(i=i):
                body(i)

    COLS = (2, 3)
    ROWS = (0, 1)

    def send_z_edges(s, again):
        if again:
            when_all(has_side, lambda d: z_send(s, d).wait_send())
        for h in range(2):
            zes[s, 2, h] = Z[s, h, 1:NB + 1, 8, :]
            zes[s, 3, h] = Z[s, h, 1:NB + 1, EX - 1, :]
        for h in range(2):
            zes[s, 0, h] = Z[s, h, 1, 8:EX, :]
            zes[s, 1, h] = Z[s, h, NB, 8:EX, :]
        when_all(has_side, lambda d: z_send(s, d).start(), COLS + ROWS)

    def stencil(s, om, first):
        @pl.loop(0, NB)
        def _(i):
            ax0 = FX[s, i, :, :]
            ax1 = FX[s, i + 1, :, :]
            ay0 = FY[s, i, 0:NB, :]
            ay1 = FY[s, i, 1:NB + 1, :]
            for h in range(2):
                zc = Z[s, h, i + 1, 8:EX, :]
                zl = Z[s, h, i + 1, 7:EX - 1, :]
                zr = Z[s, h, i + 1, 9:EX + 1, :]
                zu = Z[s, h, i, 8:EX, :]
                zd = Z[s, h, i + 2, 8:EX, :]
                av = ax0 * (zc - zu) - ax1 * (zd - zc) + ay0 * (zc - zl) - ay1 * (zr - zc)
                if first:
                    R[s, h, own_row(i), :] = U[s, h, i] - av
                    U[s, h, i] = zc
                else:
                    R[s, h, own_row(i), :] = R[s, h, own_row(i), :] - om * av
                    U[s, h, i] = U[s, h, i] + om * zc

    def stencil_rows(s, om, rows):
        for h in range(2):
            zc = Z[s, h, rows[0] + 1, 8:EX, :]
            flux = FX[s, rows[0], :, :] * (zc - Z[s, h, rows[0], 8:EX, :])
            for i in rows:
                zd = Z[s, h, i + 2, 8:EX, :]
                down = FX[s, i + 1, :, :] * (zd - zc)
                side = FY[s, i, 0:NB, :] * (zc - Z[s, h, i + 1, 7:EX - 1, :]) - FY[s, i, 1:NB + 1, :] * (Z[s, h, i + 1, 9:EX + 1, :] - zc)
                R[s, h, own_row(i), :] = R[s, h, own_row(i), :] - om * ((flux - down) + side)
                U[s, h, i] = U[s, h, i] + om * zc
                flux, zc = down, zd

    def wait_z(s, sides):
        when_all(has_side, lambda d: z_recv(s, d).wait_recv(), sides)

    def edge_fix(s, om, sides):
        for d in sides:
            for h in range(2):
                cells = (own_row(0), own_row(NB - 1), ext_col(MG), ext_col(MG + NB - 1))[d]
                R[s, h, cells, :] = R[s, h, cells, :] + om * (FE[s, d] * (zer[s, d, h] - zes[s, d, h]))

    def pack_col(s, h, d, a):
        first = MG if d == 2 else NB
        frs[s, d, a, :, pl.ds(h * LANES, LANES)] = R[s, h, ext_col(first + a), :].astype(BF16)

    def send_early(s, p, again):
        if again:
            when_all(has_side, lambda d: e_copy(s, d, OPP_SIDE[d], p).wait_send(), COLS)
        for d in COLS:
            for h in range(2):
                for a in ((1, 2, 3) if d == 2 else (0, 1, 2)):
                    pack_col(s, h, d, a)
        when_all(has_side, lambda d: e_copy(s, d, OPP_SIDE[d], p).start(), COLS)

    def send_late(s, p, again):
        if again:
            when_all(has_side, lambda d: f_copy_remote(s, d, OPP_SIDE[d], p).wait_send())
            when_all(has_corner, lambda q: k_copy(s, q, 3 - q, p).wait_send())
        for h in range(2):
            lanes = pl.ds(h * LANES, LANES)
            pack_col(s, h, 2, 0)
            pack_col(s, h, 3, 3)
            for a in range(MG):
                frs[s, 0, a, :, lanes] = R[s, h, own_row(a), :].astype(BF16)
                frs[s, 1, a, :, lanes] = R[s, h, own_row(NB - MG + a), :].astype(BF16)
            for q, (dr, dc) in enumerate(CORNERS):
                r0 = MG if dr < 0 else NB
                c0 = 0 if dc < 0 else NB
                tile = [R[s, h, pl.ds(OFF + EX * (r0 + a) + c0, 8), :] for a in range(MG)]
                crs[s, q, :, lanes] = jnp.concatenate(tile, axis=0).astype(BF16)
        when_all(has_side, lambda d: f_copy_remote(s, d, OPP_SIDE[d], p).start(), COLS + ROWS)
        when_all(has_corner, lambda q: k_copy(s, q, 3 - q, p).start())

    def wait_frames(s, p):
        when_all(has_side, lambda d: e_copy(s, OPP_SIDE[d], d, p).wait_recv(), COLS)
        when_all(has_side, lambda d: f_copy_remote(s, OPP_SIDE[d], d, p).wait_recv())
        when_all(has_corner, lambda q: k_copy(s, 3 - q, q, p).wait_recv())

    def scatter_frames(s, p):
        for d in range(4):
            for h in range(2):
                for a in range(MG):
                    cells = (own_row(a - MG), own_row(NB + a), ext_col(a), ext_col(MG + NB + a))[d]
                    R[s, h, cells, :] = frr[p, s, d, a, :, pl.ds(h * LANES, LANES)].astype(F32)
        for q, (dr, dc) in enumerate(CORNERS):
            r0 = 0 if dr < 0 else MG + NB
            for h in range(2):
                v = crr[p, s, q, :, pl.ds(h * LANES, LANES)].astype(F32)
                for a in range(MG):
                    if dc < 0:
                        R[s, h, pl.ds(OFF + EX * (r0 + a), 4), :] = v[8 * a:8 * a + 4]
                    else:
                        R[s, h, pl.ds(OFF + EX * (r0 + a) + MG + NB, 4), :] = v[8 * a + 4:8 * a + 8]

    def pair_rows(s, h, t):
        return R[s, h, pl.ds(2 * EX * t + OFF, 2 * EX), :].astype(BF16)

    def fill(s, t, tile, n, base):
        for h in range(2):
            v = R[s, h, pl.ds(2 * EX * t + 16 * tile + OFF, 16 * n), :].astype(BF16)
            W[s, pl.ds(base, 16 * n), pl.ds(h * LANES, LANES)] = v

    def fill_inner(s):
        for t in range(2, 26):
            fill(s, t, 1, 2, 64 * (t - 2))
            fill(s, t, 4, 2, 64 * (t - 2) + 32)

    def fill_frame(s):
        fill(s, 0, 0, 14, KI)
        fill(s, 26, 0, 14, KI + 224)
        for t in range(2, 26):
            for n, u in enumerate((0, 3, 6)):
                fill(s, t, u, 1, KI + 448 + 48 * (t - 2) + 16 * n)

    g = NB // CHUNKS

    def matmul(s, m, parts, k0):
        cells = pl.ds(m * rows_per, rows_per)
        lhs = [p[s, :, :, :, cells].reshape(-1, rows_per) for p in parts]
        lhs = jnp.concatenate(lhs, axis=0) if len(lhs) > 1 else lhs[0]
        z = lax.dot_general(lhs, W[s, pl.ds(k0, lhs.shape[0]), :], (((0,), (0,)), ((), ())), preferred_element_type=F32)
        return z.reshape(g, NB, 2 * LANES)

    def inner_product(s, other=None):
        fill_inner(s)
        for m in range(CHUNKS):
            if other is not None:
                stencil_rows(other, om_ref[other], range(m * g, (m + 1) * g))
            z = matmul(s, m, (SI,), 0)
            for h in range(2):
                Z[s, h, pl.ds(1 + m * g, g), 8:EX, :] = z[:, :, h * LANES:(h + 1) * LANES]

    def frame_product(s, m):
        z = matmul(s, m, (SA, SF), KI)
        return [Z[s, h, pl.ds(1 + m * g, g), 8:EX, :] + z[:, :, h * LANES:(h + 1) * LANES] for h in range(2)]

    for s in range(2):
        for h in range(2):
            u_copy(s, h).wait()
        send_z_edges(s, False)
    for first in (True, False):
        for s in range(2):
            for cp in s_copies(s, first):
                cp.start()
    for s in range(2):
        @pl.loop(0, NB)
        def _(i):
            at = pl.multiple_of(EX * i, 8)
            c_own = R[s, 0, pl.ds(at + 8, NB), :]
            FX[s, i + 1, :, :] = 0.5 * (c_own + R[s, 0, pl.ds(at + EX + 8, NB), :])
            FY[s, i, 0:NB, :] = 0.5 * (c_own + R[s, 0, pl.ds(at + 7, NB), :])

    for s in range(2):
        for d in range(4):
            face = jnp.where(has_side[d], 0.0, ces[d, s])
            if d == 0:
                FX[s, 0, :, :] = face
            elif d == 1:
                FX[s, NB, :, :] = face
            elif d == 2:
                FY[s, :, 0, :] = face
            else:
                FY[s, :, NB, :] = face

    for s in range(2):
        for h in range(2):
            f_copy(s, h).wait()
        stencil(s, None, True)
    when_all(has_side, lambda d: c_recv(d).wait_recv())
    for s in range(2):
        for d in range(4):
            FE[s, d] = jnp.where(has_side[d], 0.5 * (ces[d, s] + cer[d, s]), 0.0)
    for s in range(2):
        wait_z(s, ROWS + COLS)
        edge_fix(s, 1.0, ROWS + COLS)
        send_early(s, 0, False)
        send_late(s, 0, False)

    for s in range(2):
        for cp in s_copies(s, True):
            cp.wait()
        inner_product(s)
    for s in range(2):
        for cp in s_copies(s, False):
            cp.wait()

    def early(s, p):
        wait_z(s, ROWS)
        edge_fix(s, om_ref[s], ROWS)
        send_early(s, p, True)

    def late(s, p):
        wait_z(s, COLS)
        edge_fix(s, om_ref[s], COLS)
        send_late(s, p, True)

    def half_sweep(s, p, other, p_other, started):
        @pl.when(started)
        def _():
            early(other, p_other)
        wait_frames(s, p)
        scatter_frames(s, p)
        fill_frame(s)
        for m in range(CHUNKS):
            z = frame_product(s, m)
            for h in range(2):
                Z[s, h, pl.ds(1 + m * g, g), 8:EX, :] = z[h]
            if m == LATE_AT:
                @pl.when(started)
                def _():
                    late(other, p_other)
        send_z_edges(s, True)

    @pl.loop(0, SWEEPS - 1)
    def _(k):
        p = lax.rem(k, 2)
        half_sweep(0, p, 1, p, k > 0)

        @pl.when(k > 0)
        def _():
            inner_product(1, 0)

        @pl.when(k == 0)
        def _():
            stencil(0, om_ref[0], False)
        half_sweep(1, p, 0, 1 - p, k >= 0)
        inner_product(0, 1)

    last = (SWEEPS - 1) % 2

    def finish(s, m):
        z = frame_product(s, m)
        for h in range(2):
            U[s, h, pl.ds(m * g, g)] = U[s, h, pl.ds(m * g, g)] + om_ref[s] * z[h]

    early(1, last)
    inner_product(1)
    late(1, last)
    wait_frames(0, last)
    scatter_frames(0, last)
    fill_frame(0)
    for m in range(CHUNKS):
        finish(0, m)
    wait_frames(1, last)
    scatter_frames(1, last)
    fill_frame(1)
    for m in range(CHUNKS):
        finish(1, m)
    when_all(has_side, lambda d: c_send(d).wait_send())
    for s in range(2):
        when_all(has_side, lambda d: z_send(s, d).wait_send())
        when_all(has_side, lambda d: e_copy(s, d, OPP_SIDE[d], last).wait_send(), COLS)
        when_all(has_side, lambda d: f_copy_remote(s, d, OPP_SIDE[d], last).wait_send())
        when_all(has_corner, lambda q: k_copy(s, q, 3 - q, last).wait_send())


def write_out(u_ref, out_hbm, sem):
    def copy(s, h, m):
        g = NB // CHUNKS
        return pltpu.make_async_copy(u_ref.at[s, h, pl.ds(m * g, g)], out_hbm.at[s, pl.ds(m * g, g), :, pl.ds(h * LANES, LANES)], sem.at[s, h, m])
    for act in ("start", "wait"):
        for s in range(2):
            for h in range(2):
                for m in range(CHUNKS):
                    getattr(copy(s, h, m), act)()


def solution(mesh):
    grid_spec = P(None, "row", "col", None)

    def local(forcing, init_guess, cell_coef, solve_rows, relax_factor):
        num_sys, nb, _, rhs = forcing.shape
        s_mat = jnp.swapaxes(solve_rows, 3, 4).reshape(num_sys, EX // 2, 7, 16, nb * nb)
        any_spec = pl.BlockSpec(memory_space=pl.ANY)
        dma = pltpu.SemaphoreType.DMA
        approx = pl.pallas_call(
            kernel,
            name="schwarz",
            out_shape=pltpu.VMEM((2, 2, NB, NB, LANES), F32),
            in_specs=[any_spec, any_spec, any_spec, any_spec, pl.BlockSpec(memory_space=pltpu.SMEM)],
            out_specs=pl.BlockSpec(memory_space=pltpu.VMEM),
            scratch_shapes=[
                pltpu.VMEM((2, NB, NB), F32),
                pltpu.VMEM((2, 24, 4, 16, NB * NB), BF16),
                pltpu.VMEM((2, 4, 7, 16, NB * NB), BF16),
                pltpu.VMEM((2, 24, 3, 16, NB * NB), BF16),
                pltpu.VMEM((2, 2, 50, 64, LANES), F32),
                pltpu.VMEM((2, 2, 57 * EX, LANES), F32),
                pltpu.VMEM((2, EX * EX, 2 * LANES), BF16),
                pltpu.VMEM((2, NB + 1, NB, LANES), F32),
                pltpu.VMEM((2, NB, EX, LANES), F32),
                pltpu.VMEM((2, 4, NB, LANES), F32),
                pltpu.VMEM((4, 2, NB, LANES), F32),
                pltpu.VMEM((4, 2, NB, LANES), F32),
                pltpu.VMEM((2, 4, 2, NB, LANES), F32),
                pltpu.VMEM((2, 4, 2, NB, LANES), F32),
                pltpu.VMEM((2, 4, MG, NB, 2 * LANES), BF16),
                pltpu.VMEM((2, 2, 4, MG, NB, 2 * LANES), BF16),
                pltpu.VMEM((2, 4, 32, 2 * LANES), BF16),
                pltpu.VMEM((2, 2, 4, 32, 2 * LANES), BF16),
                dma, dma((2, 2)), dma((2, 2)), dma((2, 7)),
                dma((4,)), dma((4,)), dma((2, 4)), dma((2, 4)),
                dma((2, 4)), dma((2, 2, 4)), dma((2, 4)), dma((2, 2, 4)), dma((2, 4)), dma((2, 2, 4)),
            ],
            compiler_params=pltpu.CompilerParams(collective_id=0, has_side_effects=True, vmem_limit_bytes=61_500_000),
            cost_estimate=pl.CostEstimate(flops=30_000_000_000, bytes_accessed=43_000_000, transcendentals=0),
        )(forcing, init_guess, cell_coef, s_mat, relax_factor)
        return pl.pallas_call(
            write_out,
            name="write_out",
            out_shape=jax.ShapeDtypeStruct(forcing.shape, F32),
            in_specs=[pl.BlockSpec(memory_space=pltpu.VMEM)],
            out_specs=any_spec,
            scratch_shapes=[dma((2, 2, CHUNKS))],
            compiler_params=pltpu.CompilerParams(vmem_limit_bytes=8_000_000),
            cost_estimate=pl.CostEstimate(flops=1_000_000, bytes_accessed=9_500_000, transcendentals=0),
        )(approx)

    return jax.shard_map(local, mesh=mesh, in_specs=(grid_spec, grid_spec, P(None, "row", "col"), P(None, "row", "col", None, None), P(None)), out_specs=grid_spec, check_vma=False)
```
